128 devices in a mesh: col: 16 (over x, z), row: 8 (over y, core).
Axes of the slice: x: 4, y: 4, z: 4, core: 2. Of those that a mesh axis runs over, the one named last changes fastest.
Arguments:
- position: float32 [128, 65536], P(None, ('col', 'row')), may hold values from -6 to 6
- momentum: float32 [128, 65536], P(None, ('col', 'row')), may hold values from -6 to 6
- row_factors: bfloat16 [65536, 64, 128], P(('col', 'row')), may hold values from -1 to 1
- col_factors: bfloat16 [65536, 64, 128], P(('col', 'row')), may hold values from -1 to 1
- tile_ranks: int32 [64, 64], replicated, may hold values from 16 to 128, as said below
- log_mean: float32 [65536], P(('col', 'row')), may hold values from -0.5 to 0.5
- counts: int32 [65536], P(('col', 'row')), may hold values from 0 to 11
- step_size: float32 [128], replicated, may hold values from 0.1 to 0.3
Outputs:
- new_position: float32 [128, 65536], P(None, ('col', 'row'))
- new_momentum: float32 [128, 65536], P(None, ('col', 'row'))
- energy_change: float32 [128], replicated
The draws below stay inside these ranges and needn't reach their ends.
Inputs may be any that keep to these rules, and one draw needn't show every extreme that they name: `tile_ranks`: every entry is a multiple of 16; in every draw some tile has rank 16 and some tile has rank 128.
All inputs are finite; a program needn't handle non-finite values.
Results may differ from the reference program's by a relative error of at most 0.004.
Values may be sent and summed in bfloat16 or wider, within the bound.
No kernel may reach another device: no remote copies, remote signals or barrier semaphores. Data moves between devices by JAX's collectives and lax.ppermute only.
A program may use at most 128 MiB of HBM per device.

```python
import math
import jax
import jax.numpy as jnp
from jax import lax

TILE_CELLS = 1024
RANK_MAX = 128
RANK_BLOCK = 16
CHAINS = 128
TILES = 64
CELLS = 65536


def draw_tile_ranks(key, part):
    total = TILES * TILES
    level_count = RANK_MAX // RANK_BLOCK
    level_key = jax.random.fold_in(key, 11)
    low_key = jax.random.fold_in(key, 12)
    high_key = jax.random.fold_in(key, 13)
    drawn = jax.random.randint(level_key, (total,), 1, level_count + 1)
    low_at = jax.random.randint(low_key, (), 0, total)
    high_at = (low_at + 1 + jax.random.randint(high_key, (), 0, total - 1)) % total
    drawn = drawn.at[low_at].set(1).at[high_at].set(level_count)
    return (drawn * RANK_BLOCK).reshape(TILES, TILES).astype(jnp.int32)


def draw_counts(key, part):
    cell_index = jnp.arange(CELLS, dtype=jnp.int32)
    ceiling = 3 + 9 * cell_index // CELLS
    drawn = jax.random.randint(jax.random.fold_in(key, 21), (CELLS,), 0, 1 << 20)
    return (drawn % (ceiling + 1)).astype(jnp.int32)


def unit_entries(key, shape):
    values = jnp.clip(jax.random.normal(key, shape, jnp.float32), -6.0, 6.0)
    return values


def draw_position(key, part):
    return unit_entries(jax.random.fold_in(key, 31), (CHAINS, CELLS))


def draw_row_factors(key, part):
    values = unit_entries(jax.random.fold_in(key, 41), (CELLS, TILES, RANK_MAX))
    scale = (TILES * RANK_MAX) ** (-0.5)
    return (values * scale).astype(jnp.bfloat16)


def draw_col_factors(key, part):
    values = unit_entries(jax.random.fold_in(key, 51), (CELLS, TILES, RANK_MAX))
    scale = TILE_CELLS ** (-0.5)
    return (values * scale).astype(jnp.bfloat16)


def steps_of(own_key, dims, shards, low, largest):
    level, own = 1.0, jax.random.fold_in(own_key, 6)
    for axis_at, shards_of in shards:
        draws = jnp.exp(jax.random.uniform(jax.random.fold_in(own, axis_at), (shards_of,), jnp.float32, low / len(shards), largest / len(shards)))
        level = level * jnp.repeat(draws, dims[axis_at] // shards_of).reshape([-1 if axis == axis_at else 1 for axis in range(len(dims))])
    return level


def scatter_about(key, dims, scale, most, split=(), kind=jnp.bfloat16):
    level = steps_of(key, dims, split, -0.22, 0.18) if split else 1.0
    array = jax.random.normal(key, dims, jnp.float32) * scale * level
    return jnp.minimum(jnp.maximum(array, -most), most).astype(kind)


def setup_inputs(seed: int = 0) -> dict:
    key_list = jax.random.split(jax.random.key(seed), 9)
    return {
        "position": draw_position(jax.random.fold_in(key_list[8], 71), 0),
        "momentum": scatter_about(key_list[1], (CHAINS, CELLS), 1.0, 6.0, ((1, 128),), jnp.float32),
        "row_factors": draw_row_factors(jax.random.fold_in(key_list[8], 71), 0),
        "col_factors": draw_col_factors(jax.random.fold_in(key_list[8], 71), 0),
        "tile_ranks": draw_tile_ranks(jax.random.fold_in(key_list[8], 71), 0),
        "log_mean": jnp.clip(jax.random.uniform(key_list[5], (CELLS,), jnp.float32, -0.5, 0.5) * steps_of(key_list[5], (CELLS,), ((0, 128),), -0.4, 0.0), -0.5, 0.5),
        "counts": draw_counts(jax.random.fold_in(key_list[8], 71), 0),
        "step_size": jnp.clip(jnp.exp(jax.random.uniform(key_list[7], (CHAINS,), jnp.float32, math.log(0.1), math.log(0.3))), 0.1, 0.3),
    }


def half_round(values):
    return lax.optimization_barrier(values.astype(jnp.bfloat16)).astype(jnp.float32)


def gradient(position, row_factors, col_factors, alive_mask, log_mean, counts):
    chains = position.shape[0]
    half_cells = TILE_CELLS // 2
    cell_grid = half_round(position).reshape(chains, TILES, 2, half_cells)
    col_grid = col_factors.reshape(TILES, 2, half_cells, TILES, RANK_MAX)
    row_grid = row_factors.reshape(TILES, 2, half_cells, TILES, RANK_MAX)
    tile_order = jnp.arange(TILES, dtype=jnp.int32)

    def forward(column):
        factor_block = col_grid[column].astype(jnp.float32)
        values = cell_grid[:, column]
        partial_value = jnp.einsum('syik,hsy->sikh', factor_block, values)
        partial_value = half_round(partial_value * alive_mask[:, column][None, :, :, None])
        return half_round(partial_value[0] + partial_value[1])

    coefficients = lax.map(forward, tile_order)

    def field_rows(tile_index):
        factor_block = row_grid[tile_index].astype(jnp.float32)
        coefficient = coefficients[:, tile_index]
        return jnp.einsum('sxjk,jkh->hsx', factor_block, coefficient)

    latent_field = lax.map(field_rows, tile_order)
    latent_field = jnp.transpose(latent_field, (1, 0, 2, 3)).reshape(chains, CELLS)
    exponent = log_mean[None, :] + latent_field
    intensity = jnp.exp(exponent)
    rate_base = counts.astype(jnp.float32)[None, :]
    residual = rate_base - intensity
    residual_grid = half_round(residual).reshape(chains, TILES, 2, half_cells)

    def backward(tile_index):
        factor_block = row_grid[tile_index].astype(jnp.float32)
        values = residual_grid[:, tile_index]
        partial_value = jnp.einsum('sxjk,hsx->sjkh', factor_block, values)
        partial_value = half_round(partial_value * alive_mask[tile_index][None, :, :, None])
        return half_round(partial_value[0] + partial_value[1])

    returned = lax.map(backward, tile_order)

    def pull_columns(column):
        factor_block = col_grid[column].astype(jnp.float32)
        coefficient = returned[:, column]
        return jnp.einsum('syik,ikh->hsy', factor_block, coefficient)

    pulled = lax.map(pull_columns, tile_order)
    pulled = jnp.transpose(pulled, (1, 0, 2, 3)).reshape(chains, CELLS)
    pieces = intensity - rate_base * exponent + 0.5 * position * position
    return position - pulled, pieces


def reference(position, momentum, row_factors, col_factors, tile_ranks, log_mean, counts, step_size):
    levels = jnp.arange(RANK_MAX, dtype=jnp.int32)
    alive_mask = (levels[None, None, :] < tile_ranks[:, :, None]).astype(jnp.float32)
    half_step = 0.5 * step_size[:, None]
    full_step = step_size[:, None]
    forces, start_energy = gradient(position, row_factors, col_factors, alive_mask, log_mean, counts)
    moment = momentum - half_step * forces
    shifted = position + full_step * moment
    forces, unused = gradient(shifted, row_factors, col_factors, alive_mask, log_mean, counts)
    moment = moment - full_step * forces
    shifted = shifted + full_step * moment
    forces, end_energy = gradient(shifted, row_factors, col_factors, alive_mask, log_mean, counts)
    moment = moment - half_step * forces
    change = jnp.sum(end_energy - start_energy + 0.5 * (moment * moment - momentum * momentum), axis=1)
    return shifted, moment, change
```

```python
import functools

import jax
import jax.numpy as jnp
from jax import lax
from jax.experimental import pallas as pl
from jax.experimental.pallas import tpu as pltpu
from jax.sharding import Mesh
from jax.sharding import PartitionSpec as P

COL_ROW = ("col_0", "col_1", "row_0", "row_1")
CHIPS = ("col_0", "col_1", "row_0")
CORE = "row_1"
BF16 = jnp.bfloat16
F32 = jnp.float32
LIMIT = 8 << 20
NT = (((1,), (1,)), ((), ()))
VMEM = pl.BlockSpec(memory_space=pltpu.VMEM)
SMEM = pl.BlockSpec(memory_space=pltpu.SMEM)
ANY = pl.BlockSpec(memory_space=pl.ANY)


def swap(value):
    return lax.ppermute(value, CORE, [(0, 1), (1, 0)])


def spread(value):
    return lax.all_to_all(value, CHIPS, split_axis=0, concat_axis=0, tiled=True)


def other_half(value):
    lanes = value.shape[1] // 2
    return jnp.concatenate([value[:, lanes:], value[:, :lanes]], axis=1)


def low_lanes(value):
    return lax.broadcasted_iota(jnp.int32, value.shape, 1) < value.shape[1] // 2


def regroup_kernel(tiles, core_ref, raw_ref, own_ref, send_ref):
    to = lax.broadcasted_iota(jnp.int32, (256, 256), 0)
    at = lax.broadcasted_iota(jnp.int32, (256, 256), 1)
    order = (at == (to % 16) * 16 + to // 16).astype(F32).astype(BF16)
    first_core = core_ref[0] == 0
    cells = raw_ref.shape[0] // tiles

    def group(index, carry):
        first = index * 16
        at_cell = pl.ds(pl.multiple_of(first, 16), 16)
        for block in range(2):
            sides = []
            for side in range(2):
                rows = [
                    raw_ref[pl.ds(pl.multiple_of((first + y) * tiles, 16) + (2 * block + side) * 16, 16), :]
                    for y in range(16)
                ]
                sides.append(jnp.concatenate(rows, axis=0))
            low = low_lanes(sides[0])
            halves = [
                jnp.where(low, sides[0], other_half(sides[1])),
                jnp.where(low, other_half(sides[0]), sides[1]),
            ]
            own = jnp.where(first_core, halves[0], halves[1])
            send = jnp.where(first_core, halves[1], halves[0])
            moved = jnp.dot(
                order, jnp.concatenate([own, send], axis=1), preferred_element_type=F32
            ).astype(BF16)
            lanes = slice(block * 128, block * 128 + 128)
            for q in range(16):
                own_ref[q, at_cell, lanes] = moved[q * 16 : (q + 1) * 16, :128]
                send_ref[q, at_cell, lanes] = moved[q * 16 : (q + 1) * 16, 128:]
        return carry

    lax.fori_loop(0, cells // 16, group, 0, unroll=2)


def regroup(factors, core):
    cells, tiles, ranked = factors.shape
    step = 64
    quads = tiles // 4
    shape = pltpu.HBM((quads, cells, 2 * ranked), BF16)
    block = pl.BlockSpec((quads, step, 2 * ranked), lambda g: (0, g, 0))
    return pl.pallas_call(
        functools.partial(regroup_kernel, tiles),
        grid=(cells // step,),
        in_specs=[SMEM, pl.BlockSpec((step * tiles, ranked), lambda g: (g, 0))],
        out_specs=[block, block],
        out_shape=[shape, shape],
        compiler_params=pltpu.CompilerParams(vmem_limit_bytes=12 << 20),
        cost_estimate=pl.CostEstimate(
            flops=8_000_000_000, bytes_accessed=1 << 24, transcendentals=0
        ),
    )(core, pltpu.with_memory_space_constraint(factors.reshape(cells * tiles, ranked), pltpu.HBM))


def merge_kernel(after_ref, own_ref, other_ref, out_ref, sems):
    copies = [
        pltpu.make_async_copy(ref, out_ref.at[side], sems.at[side])
        for side, ref in enumerate((own_ref, other_ref))
    ]
    for copy in copies:
        copy.start()
    for copy in copies:
        copy.wait()


def merge(after, own, other):
    return pl.pallas_call(
        merge_kernel,
        in_specs=[ANY, ANY, ANY],
        out_specs=VMEM,
        out_shape=jax.ShapeDtypeStruct((2, *own.shape), own.dtype),
        scratch_shapes=[pltpu.SemaphoreType.DMA((2,))],
        compiler_params=pltpu.CompilerParams(vmem_limit_bytes=1 << 20),
        cost_estimate=pl.CostEstimate(
            flops=4_000_000_000, bytes_accessed=1 << 24, transcendentals=0
        ),
    )(after, *[pltpu.with_memory_space_constraint(f, pltpu.HBM) for f in (own, other)])


def expand_kernel(coefficient_ref, f_ref, total_ref, left):
    quads, cells = f_ref.shape[1], f_ref.shape[2]
    half = coefficient_ref.shape[1]

    def arrange(q, carry):
        for pair in range(2):
            one = coefficient_ref[q + 32 * pair]
            two = coefficient_ref[q + 32 * pair + 16]
            low = low_lanes(one)
            lanes = slice(pair * 128, pair * 128 + 128)
            left[q, :half, lanes] = jnp.where(low, one, other_half(two))
            left[q, half:, lanes] = jnp.where(low, other_half(one), two)
        return carry

    lax.fori_loop(0, quads, arrange, 0, unroll=2)
    for side in range(2):
        def block(index, carry):
            at_cell = pl.ds(pl.multiple_of(index * 256, 256), 256)
            total_ref[:, pl.ds(pl.multiple_of(side * cells + index * 256, 256), 256)] = sum(
                lax.dot_general(
                    left[q], f_ref[side, q, at_cell, :], NT, preferred_element_type=F32
                )
                for q in range(quads)
            )
            return carry

        lax.fori_loop(0, cells // 256, block, 0, unroll=2)


def project(values, f_ref, core_ref, ranks_ref, out_ref):
    quads, cells = f_ref.shape[1], f_ref.shape[2]
    half = out_ref.shape[1]
    lane = lax.broadcasted_iota(jnp.int32, (2 * half, 128), 1)
    low = lane < 64
    level = lane % 64 + 64 * core_ref[0]
    low_rows = low[:half]

    def quad(q, carry):
        moved = jnp.dot(
            values[:, :cells], f_ref[0, q], preferred_element_type=F32
        ) + jnp.dot(values[:, cells:], f_ref[1, q], preferred_element_type=F32)
        for pair in range(2):
            one, two = q + 32 * pair, q + 32 * pair + 16
            ranks = jnp.where(low, ranks_ref[one], ranks_ref[two])
            part = moved[:, pair * 128 : pair * 128 + 128]
            part = jnp.where(level < ranks, part, 0.0).astype(BF16)
            turned = other_half(part)
            out_ref[one] = jnp.where(low_rows, part[:half], turned[half:])
            out_ref[two] = jnp.where(low_rows, turned[:half], part[half:])
        return carry

    lax.fori_loop(0, quads, quad, 0, unroll=4)


def complete(total_ref, arrived_ref):
    cells = total_ref.shape[1] // 2
    return [
        total_ref[:, :cells] + arrived_ref[:, cells:],
        total_ref[:, cells:] + arrived_ref[:, :cells],
    ]


def first_kernel(core_ref, ranks_ref, z0_ref, z1_ref, f_ref, out_ref, values):
    cells = z0_ref.shape[1]
    values[:, :cells] = z0_ref[...].astype(BF16)
    values[:, cells:] = z1_ref[...].astype(BF16)
    project(values, f_ref, core_ref, ranks_ref, out_ref)


def row_kernel(
    core_ref, ranks_ref, total_ref, arrived_ref, base_ref, rate_ref, f_ref,
    out_ref, energy_ref, values,
):
    cells = total_ref.shape[1] // 2
    for side, field in enumerate(complete(total_ref, arrived_ref)):
        at = slice(side * cells, (side + 1) * cells)
        rate = rate_ref[:, at]
        exponent = base_ref[:, at] + field
        intensity = jnp.exp(exponent)
        values[:, at] = (rate - intensity).astype(BF16)
        if side == 0:
            energy_ref[...] = jnp.sum(intensity - rate * exponent, axis=1, keepdims=True)
    project(values, f_ref, core_ref, ranks_ref, out_ref)


def col_kernel(
    weight, core_ref, ranks_ref, total_ref, arrived_ref, step_ref, z_ref, m_ref,
    f_ref, out_ref, new_z_ref, new_m_ref, values,
):
    cells = total_ref.shape[1] // 2
    step = step_ref[:, :1]
    for side, pulled in enumerate(complete(total_ref, arrived_ref)):
        at = slice(side * cells, (side + 1) * cells)
        z = z_ref[:, at]
        moment = m_ref[:, at] - weight * step * (z - pulled)
        z = z + step * moment
        new_m_ref[:, at] = moment
        new_z_ref[:, at] = z
        values[:, at] = z.astype(BF16)
    project(values, f_ref, core_ref, ranks_ref, out_ref)


def last_kernel(
    total_ref, arrived_ref, step_ref, z_ref, m_ref, start_z_ref, start_m_ref,
    start_energy_ref, end_energy_ref, new_m_ref, change_ref,
):
    cells = total_ref.shape[1] // 2
    z = z_ref[:, :cells]
    moment = m_ref[:, :cells] - 0.5 * step_ref[:, :1] * (
        z - complete(total_ref, arrived_ref)[0]
    )
    new_m_ref[...] = moment
    start_z = start_z_ref[:, :cells]
    start_m = start_m_ref[:, :cells]
    pieces = 0.5 * (z * z - start_z * start_z + moment * moment - start_m * start_m)
    change_ref[...] = (
        jnp.sum(pieces, axis=1, keepdims=True) + end_energy_ref[...] - start_energy_ref[...]
    )


def call(kernel, specs, outs, scratch, flops, *args):
    return pl.pallas_call(
        kernel,
        in_specs=specs,
        out_specs=[VMEM] * len(outs),
        out_shape=[jax.ShapeDtypeStruct(*o) for o in outs],
        scratch_shapes=scratch,
        compiler_params=pltpu.CompilerParams(vmem_limit_bytes=LIMIT),
        cost_estimate=pl.CostEstimate(
            flops=flops, bytes_accessed=1 << 24, transcendentals=0
        ),
    )(*args)


def on_device(
    position, momentum, row_factors, col_factors, tile_ranks, log_mean, counts, step_size
):
    chains, cells = position.shape
    half = chains // 2
    tiles, ranked = tile_ranks.shape[0], row_factors.shape[2]
    tile = lax.axis_index(CHIPS)
    core = lax.axis_index(CORE).astype(jnp.int32)[None]
    col_ranks = lax.dynamic_slice_in_dim(tile_ranks, tile, 1, 1)[:, 0]
    row_ranks = lax.dynamic_slice_in_dim(tile_ranks, tile, 1, 0)[0]

    coefficients = ((tiles, half, ranked), BF16)
    state = ((chains, 2 * cells), F32)
    own_state = ((chains, cells), F32)
    column = ((chains, 1), F32)
    values = [pltpu.VMEM((chains, 2 * cells), BF16)]
    left = [pltpu.VMEM((tiles // 4, chains, 2 * ranked), BF16)]
    work = 2 * chains * 2 * cells * tiles * ranked // 2

    z_other = swap(position)
    own, send = regroup(col_factors, core)
    send, z_other = lax.optimization_barrier((send, z_other))
    col = merge(z_other, own, swap(send))
    row_own, send = regroup(row_factors, core)
    row_other = swap(send)
    start_z = jnp.concatenate([position, z_other], axis=1)
    start_m = jnp.concatenate([momentum, swap(momentum)], axis=1)
    rate = counts.astype(F32)
    base = jnp.concatenate([log_mean, swap(log_mean)])[None, :]
    rate = jnp.concatenate([rate, swap(rate)])[None, :]
    step = jnp.broadcast_to(step_size[:, None], (chains, ranked))

    def expand(coefficient, factors):
        (total,) = call(
            expand_kernel, [VMEM] * 2, [state], left, 2 * work, coefficient, factors
        )
        return total, swap(total)

    def row_pass(arrived):
        return call(
            row_kernel, [SMEM] * 2 + [VMEM] * 5, [coefficients, column], values, work,
            core, row_ranks, *expand(arrived, row), base, rate, row,
        )

    (out,) = call(
        first_kernel, [SMEM] * 2 + [VMEM] * 3, [coefficients], values, work,
        core, col_ranks, position, z_other, col,
    )
    out, start_z, start_m, base, rate, step, row_ranks = lax.optimization_barrier(
        (out, start_z, start_m, base, rate, step, row_ranks)
    )
    z, m = start_z, start_m
    arrived = spread(out)
    row = merge(arrived, row_own, row_other)
    out, start_energy = row_pass(arrived)
    for weight in (0.5, 1.0):
        out, z, m = call(
            functools.partial(col_kernel, weight),
            [SMEM] * 2 + [VMEM] * 6, [coefficients, state, state], values, work,
            core, col_ranks, *expand(spread(out), col), step, z, m, col,
        )
        out, end_energy = row_pass(spread(out))
    m, change = call(
        last_kernel, [VMEM] * 9, [own_state, column], [], 1 << 24,
        *expand(spread(out), col), step, z, m, start_z, start_m,
        start_energy, end_energy,
    )
    change = change[:, 0]
    change = change + swap(change)
    change = spread(jnp.broadcast_to(change[None], (tiles, chains))).sum(axis=0)
    return z[:, :cells], m, change


def solution(mesh):
    split = Mesh(
        mesh.devices.reshape(4, 4, 4, 2), ("col_0", "col_1", "row_0", "row_1")
    )
    return jax.shard_map(
        on_device,
        mesh=split,
        in_specs=(
            P(None, COL_ROW),
            P(None, COL_ROW),
            P(COL_ROW, None, None),
            P(COL_ROW, None, None),
            P(),
            P(COL_ROW),
            P(COL_ROW),
            P(),
        ),
        out_specs=(P(None, COL_ROW), P(None, COL_ROW), P()),
        check_vma=False,
    )
```

```python
import functools

import jax
import jax.numpy as jnp
from jax import lax
from jax.experimental import pallas as pl
from jax.experimental.pallas import tpu as pltpu
from jax.sharding import Mesh
from jax.sharding import PartitionSpec as P

COL_ROW = ("col_0", "col_1", "row_0", "row_1")
CHIPS = ("col_0", "col_1", "row_0")
CORE = "row_1"
BF16 = jnp.bfloat16
F32 = jnp.float32
LIMIT = 8 << 20
UNROLL = 8
NT = (((1,), (1,)), ((), ()))
VMEM = pl.BlockSpec(memory_space=pltpu.VMEM)
SMEM = pl.BlockSpec(memory_space=pltpu.SMEM)
ANY = pl.BlockSpec(memory_space=pl.ANY)


def swap(value):
    return lax.ppermute(value, CORE, [(0, 1), (1, 0)])


def spread(value):
    return lax.all_to_all(value, CHIPS, split_axis=0, concat_axis=0, tiled=True)


def in_hbm(value):
    return pltpu.with_memory_space_constraint(value, pltpu.HBM)


def other_half(value):
    lanes = value.shape[1] // 2
    return jnp.concatenate([value[:, lanes:], value[:, :lanes]], axis=1)


def low_lanes(value):
    return lax.broadcasted_iota(jnp.int32, value.shape, 1) < value.shape[1] // 2


def regroup_kernel(first, core_ref, raw_ref, *refs):
    if first:
        z_ref, own_live_ref, sent_live_ref, *refs = refs
    own_ref, sent_ref, *refs = refs
    if first:
        keep_ref, send_ref, *refs = refs
    raw, own, sent, in_sems, out_sems, *refs = refs
    quads, cells, _ = own.shape
    tiles = 4 * quads
    step = cells // in_sems.shape[0]

    def arrival(piece):
        rows = pl.ds(pl.multiple_of(piece * step * tiles, 16), step * tiles)
        return pltpu.make_async_copy(raw_ref.at[rows], raw.at[rows], in_sems.at[piece])

    def departures(piece):
        at = pl.ds(pl.multiple_of(piece * step, 16), step)
        return [
            pltpu.make_async_copy(
                held.at[:, at, :], ref.at[:, at, :], out_sems.at[side, piece]
            )
            for side, (held, ref) in enumerate(((own, own_ref), (sent, sent_ref)))
        ]

    def launch(piece, carry):
        arrival(piece).start()
        return carry

    lax.fori_loop(0, in_sems.shape[0], launch, 0)
    to = lax.broadcasted_iota(jnp.int32, (256, 256), 0)
    at = lax.broadcasted_iota(jnp.int32, (256, 256), 1)
    order = (at == (to % 16) * 16 + to // 16).astype(F32).astype(BF16)
    first_core = core_ref[0] == 0

    def turn(piece, carry):
        arrival(piece).wait()
        for group in range(step // 16):
            cell = pl.multiple_of(piece * step + group * 16, 16)
            for block in range(2):
                sides = [
                    jnp.concatenate(
                        [
                            raw[pl.ds(pl.multiple_of((cell + y) * tiles + (2 * block + side) * 16, 16), 16), :]
                            for y in range(16)
                        ],
                        axis=0,
                    )
                    for side in range(2)
                ]
                low = low_lanes(sides[0])
                halves = [
                    jnp.where(low, sides[0], other_half(sides[1])),
                    jnp.where(low, other_half(sides[0]), sides[1]),
                ]
                both = jnp.concatenate(
                    [
                        jnp.where(first_core, halves[0], halves[1]),
                        jnp.where(first_core, halves[1], halves[0]),
                    ],
                    axis=1,
                )
                moved = jnp.dot(order, both, preferred_element_type=F32).astype(BF16)
                lanes = slice(block * 128, block * 128 + 128)
                for q in range(16):
                    own[q, pl.ds(cell, 16), lanes] = moved[q * 16 : (q + 1) * 16, :128]
                    sent[q, pl.ds(cell, 16), lanes] = moved[q * 16 : (q + 1) * 16, 128:]
        for copy in departures(piece):
            copy.start()
        return carry

    lax.fori_loop(0, in_sems.shape[0], turn, 0)
    if first:
        (values,) = refs
        values[...] = z_ref[...].astype(BF16)
        for held, live_ref, out_ref in (
            (sent, sent_live_ref, send_ref),
            (own, own_live_ref, keep_ref),
        ):
            def factor(q):
                return jnp.dot(values[...], held[q], preferred_element_type=F32)

            project(factor, quads, live_ref, out_ref)

    def finish(piece, carry):
        for copy in departures(piece):
            copy.wait()
        return carry

    lax.fori_loop(0, in_sems.shape[0], finish, 0)


def regroup(factors, core, z=None, lives=(), coefficients=None):
    cells, tiles, ranked = factors.shape
    quads = tiles // 4
    first = z is not None
    shape = (quads, cells, 2 * ranked)
    parts = 8
    scratch = [
        pltpu.VMEM((cells * tiles, ranked), BF16),
        pltpu.VMEM(shape, BF16),
        pltpu.VMEM(shape, BF16),
        pltpu.SemaphoreType.DMA((parts,)),
        pltpu.SemaphoreType.DMA((2, parts)),
    ]
    if first:
        scratch.append(pltpu.VMEM(z.shape, BF16))
    return pl.pallas_call(
        functools.partial(regroup_kernel, first),
        in_specs=[SMEM, ANY] + [VMEM] * (3 if first else 0),
        out_specs=[ANY] * 2 + [VMEM] * (2 if first else 0),
        out_shape=[pltpu.HBM(shape, BF16)] * 2
        + ([jax.ShapeDtypeStruct(*coefficients)] * 2 if first else []),
        scratch_shapes=scratch,
        compiler_params=pltpu.CompilerParams(vmem_limit_bytes=24 << 20),
        cost_estimate=pl.CostEstimate(
            flops=8_000_000_000, bytes_accessed=1 << 24, transcendentals=0
        ),
    )(core, in_hbm(factors.reshape(cells * tiles, ranked)), *((z, *lives) if first else ()))


def merge_kernel(after_ref, own_ref, other_ref, out_ref, sems):
    copies = [
        pltpu.make_async_copy(ref, out_ref.at[side], sems.at[side])
        for side, ref in enumerate((own_ref, other_ref))
    ]
    for copy in copies:
        copy.start()
    for copy in copies:
        copy.wait()


def merge(after, own, other):
    return pl.pallas_call(
        merge_kernel,
        in_specs=[ANY, ANY, ANY],
        out_specs=VMEM,
        out_shape=jax.ShapeDtypeStruct((2, *own.shape), own.dtype),
        scratch_shapes=[pltpu.SemaphoreType.DMA((2,))],
        compiler_params=pltpu.CompilerParams(vmem_limit_bytes=1 << 20),
        cost_estimate=pl.CostEstimate(
            flops=4_000_000_000, bytes_accessed=1 << 24, transcendentals=0
        ),
    )(after, in_hbm(own), in_hbm(other))


def expand_kernel(coefficient_ref, f_ref, total_ref, left):
    quads, cells = f_ref.shape[1], f_ref.shape[2]
    half = coefficient_ref.shape[1]

    def arrange(q, carry):
        for pair in range(2):
            one = coefficient_ref[q + 32 * pair]
            two = coefficient_ref[q + 32 * pair + 16]
            low = low_lanes(one)
            lanes = slice(pair * 128, pair * 128 + 128)
            left[q, :half, lanes] = jnp.where(low, one, other_half(two))
            left[q, half:, lanes] = jnp.where(low, other_half(one), two)
        return carry

    lax.fori_loop(0, quads, arrange, 0, unroll=2)
    for side in range(2):
        def block(index, carry):
            at_cell = pl.ds(pl.multiple_of(index * 256, 256), 256)
            total_ref[:, pl.ds(pl.multiple_of(side * cells + index * 256, 256), 256)] = sum(
                lax.dot_general(
                    left[q], f_ref[side, q, at_cell, :], NT, preferred_element_type=F32
                )
                for q in range(quads)
            )
            return carry

        lax.fori_loop(0, cells // 256, block, 0, unroll=2)


def project(factor, quads, live_ref, out_ref):
    half = out_ref.shape[1]
    low = lax.broadcasted_iota(jnp.int32, (half, 128), 1) < 64

    def quad(q, carry):
        moved = factor(q)
        for pair in range(2):
            one, two = q + 32 * pair, q + 32 * pair + 16
            part = moved[:, pair * 128 : pair * 128 + 128] * live_ref[pair * 16 + q, :1]
            part = part.astype(BF16)
            turned = other_half(part)
            out_ref[one] = jnp.where(low, part[:half], turned[half:])
            out_ref[two] = jnp.where(low, turned[:half], part[half:])
        return carry

    lax.fori_loop(0, quads, quad, 0, unroll=UNROLL)


def project_both(values, f_ref, live_ref, out_ref):
    cells = f_ref.shape[2]

    def factor(q):
        return jnp.dot(
            values[:, :cells], f_ref[0, q], preferred_element_type=F32
        ) + jnp.dot(values[:, cells:], f_ref[1, q], preferred_element_type=F32)

    project(factor, f_ref.shape[1], live_ref, out_ref)


def complete(total_ref, arrived_ref):
    cells = total_ref.shape[1] // 2
    return [
        total_ref[:, :cells] + arrived_ref[:, cells:],
        total_ref[:, cells:] + arrived_ref[:, :cells],
    ]


def row_kernel(
    live_ref, total_ref, arrived_ref, base_ref, rate_ref, f_ref,
    out_ref, *refs,
):
    *energy_ref, values = refs
    cells = total_ref.shape[1] // 2
    for side, field in enumerate(complete(total_ref, arrived_ref)):
        at = slice(side * cells, (side + 1) * cells)
        rate = rate_ref[:, at]
        exponent = base_ref[:, at] + field
        intensity = jnp.exp(exponent)
        values[:, at] = (rate - intensity).astype(BF16)
        if side == 0 and energy_ref:
            energy_ref[0][...] = jnp.sum(intensity - rate * exponent, axis=1, keepdims=True)
    project_both(values, f_ref, live_ref, out_ref)


def col_kernel(
    weight, live_ref, total_ref, arrived_ref, step_ref, z_ref, m_ref,
    f_ref, out_ref, new_z_ref, new_m_ref, values,
):
    cells = total_ref.shape[1] // 2
    step = step_ref[:, :1]
    for side, pulled in enumerate(complete(total_ref, arrived_ref)):
        at = slice(side * cells, (side + 1) * cells)
        z = z_ref[:, at]
        moment = m_ref[:, at] - weight * step * (z - pulled)
        z = z + step * moment
        new_m_ref[:, at] = moment
        new_z_ref[:, at] = z
        values[:, at] = z.astype(BF16)
    project_both(values, f_ref, live_ref, out_ref)


def last_kernel(
    total_ref, arrived_ref, step_ref, z_ref, m_ref, start_z_ref, start_m_ref,
    start_energy_ref, end_energy_ref, new_m_ref, change_ref,
):
    cells = total_ref.shape[1] // 2
    z = z_ref[:, :cells]
    moment = m_ref[:, :cells] - 0.5 * step_ref[:, :1] * (
        z - complete(total_ref, arrived_ref)[0]
    )
    new_m_ref[...] = moment
    start_z = start_z_ref[:, :cells]
    start_m = start_m_ref[:, :cells]
    pieces = 0.5 * (z * z - start_z * start_z + moment * moment - start_m * start_m)
    change_ref[...] = (
        jnp.sum(pieces, axis=1, keepdims=True) + end_energy_ref[...] - start_energy_ref[...]
    )


def call(kernel, specs, outs, scratch, flops, *args):
    return pl.pallas_call(
        kernel,
        in_specs=specs,
        out_specs=[VMEM] * len(outs),
        out_shape=[jax.ShapeDtypeStruct(*o) for o in outs],
        scratch_shapes=scratch,
        compiler_params=pltpu.CompilerParams(vmem_limit_bytes=LIMIT),
        cost_estimate=pl.CostEstimate(
            flops=flops, bytes_accessed=1 << 24, transcendentals=0
        ),
    )(*args)


def on_device(
    position, momentum, row_factors, col_factors, tile_ranks, log_mean, counts, step_size
):
    chains, cells = position.shape
    half = chains // 2
    tiles, ranked = tile_ranks.shape[0], row_factors.shape[2]
    tile = lax.axis_index(CHIPS)
    core = lax.axis_index(CORE).astype(jnp.int32)[None]
    lane = jnp.arange(ranked, dtype=jnp.int32)

    def live(ranks, which):
        tops = ranks.reshape(2, 2, tiles // 4)
        top = jnp.where(lane < ranked // 2, tops[:, 0, :, None], tops[:, 1, :, None])
        level = lane % (ranked // 2) + ranked // 2 * which
        alive = (level < top).astype(F32).reshape(tiles // 2, 1, ranked)
        return jnp.broadcast_to(alive, (tiles // 2, 8, ranked))

    col_ranks = lax.dynamic_slice_in_dim(tile_ranks, tile, 1, 1)[:, 0]
    row_ranks = lax.dynamic_slice_in_dim(tile_ranks, tile, 1, 0)[0]
    col_live, sent_live = live(col_ranks, core[0]), live(col_ranks, 1 - core[0])
    row_live = live(row_ranks, core[0])

    coefficients = ((tiles, half, ranked), BF16)
    state = ((chains, 2 * cells), F32)
    own_state = ((chains, cells), F32)
    column = ((chains, 1), F32)
    values = [pltpu.VMEM((chains, 2 * cells), BF16)]
    left = [pltpu.VMEM((tiles // 4, chains, 2 * ranked), BF16)]
    work = 2 * chains * 2 * cells * tiles * ranked // 2

    z_other = swap(position)
    col_own, col_sent, keep, send = regroup(
        col_factors, core, position, (col_live, sent_live), coefficients
    )
    arrived = swap(send)
    out = (keep.astype(F32) + arrived.astype(F32)).astype(BF16)
    start_z = jnp.concatenate([position, z_other], axis=1)
    start_m = jnp.concatenate([momentum, swap(momentum)], axis=1)
    rate = counts.astype(F32)
    base = jnp.concatenate([log_mean, swap(log_mean)])[None, :]
    rate = jnp.concatenate([rate, swap(rate)])[None, :]
    step = jnp.broadcast_to(step_size[:, None], (chains, ranked))

    def expand(coefficient, factors):
        (total,) = call(
            expand_kernel, [VMEM] * 2, [state], left, 2 * work, coefficient, factors
        )
        return total, swap(total)

    def row_pass(arrived, energy=True):
        return call(
            row_kernel, [VMEM] * 6, [coefficients] + [column] * energy, values, work,
            row_live, *expand(arrived, row), base, rate, row,
        )

    col_sent, out, start_z, start_m, base, rate, step, row_live, row_raw = (
        lax.optimization_barrier(
            (col_sent, out, start_z, start_m, base, rate, step, row_live, row_factors)
        )
    )
    row_own, row_sent = regroup(row_raw, core)
    row_other = swap(row_sent)
    col_other = swap(col_sent)
    z, m = start_z, start_m
    arrived = spread(out)
    row = merge(arrived, row_own, row_other)
    out, start_energy = row_pass(arrived)
    out, col_other = lax.optimization_barrier((out, col_other))
    arrived = spread(out)
    col = merge(arrived, col_own, col_other)
    for weight in (0.5, 1.0):
        out, z, m = call(
            functools.partial(col_kernel, weight),
            [VMEM] * 7, [coefficients, state, state], values, work,
            col_live, *expand(arrived, col), step, z, m, col,
        )
        last = weight == 1.0
        out, *energy = row_pass(spread(out), last)
        arrived = spread(out)
    (end_energy,) = energy
    m, change = call(
        last_kernel, [VMEM] * 9, [own_state, column], [], 1 << 24,
        *expand(arrived, col), step, z, m, start_z, start_m,
        start_energy, end_energy,
    )
    change = change[:, 0]
    change = change + swap(change)
    change = spread(jnp.broadcast_to(change[None], (tiles, chains))).sum(axis=0)
    return z[:, :cells], m, change


def solution(mesh):
    split = Mesh(
        mesh.devices.reshape(4, 4, 4, 2), ("col_0", "col_1", "row_0", "row_1")
    )
    return jax.shard_map(
        on_device,
        mesh=split,
        in_specs=(
            P(None, COL_ROW),
            P(None, COL_ROW),
            P(COL_ROW, None, None),
            P(COL_ROW, None, None),
            P(),
            P(COL_ROW),
            P(COL_ROW),
            P(),
        ),
        out_specs=(P(None, COL_ROW), P(None, COL_ROW), P()),
        check_vma=False,
    )
```

```python
import functools

import jax
import jax.numpy as jnp
from jax import lax
from jax.experimental import pallas as pl
from jax.experimental.pallas import tpu as pltpu
from jax.sharding import Mesh
from jax.sharding import PartitionSpec as P

COL_ROW = ("col_0", "col_1", "row_0", "row_1")
CHIPS = ("col_0", "col_1", "row_0")
CORE = "row_1"
BF16 = jnp.bfloat16
F32 = jnp.float32
LIMIT = 8 << 20
UNROLL = 8
NT = (((1,), (1,)), ((), ()))
VMEM = pl.BlockSpec(memory_space=pltpu.VMEM)
SMEM = pl.BlockSpec(memory_space=pltpu.SMEM)
ANY = pl.BlockSpec(memory_space=pl.ANY)


def swap(value):
    return lax.ppermute(value, CORE, [(0, 1), (1, 0)])


def spread(value):
    return lax.all_to_all(value, CHIPS, split_axis=0, concat_axis=0, tiled=True)


def in_hbm(value):
    return pltpu.with_memory_space_constraint(value, pltpu.HBM)


def other_half(value):
    lanes = value.shape[1] // 2
    return jnp.concatenate([value[:, lanes:], value[:, :lanes]], axis=1)


def low_lanes(value):
    return lax.broadcasted_iota(jnp.int32, value.shape, 1) < value.shape[1] // 2


def one_hot(index):
    to = lax.broadcasted_iota(jnp.int32, (256, 256), 0)
    at = lax.broadcasted_iota(jnp.int32, (256, 256), 1)
    return (at == index(to)).astype(F32).astype(BF16)


def tile_major(to):
    return (to % 16) * 16 + to // 16


def read_blocks(raw, cell, tiles):
    return [
        jnp.concatenate(
            [
                raw[pl.ds(pl.multiple_of((cell + y) * tiles + block * 16, 16), 16), :]
                for y in range(16)
            ],
            axis=0,
        )
        for block in range(tiles // 16)
    ]


def half_lanes(one, two, which):
    low = low_lanes(one)
    if which == 0:
        return jnp.where(low, one, other_half(two))
    return jnp.where(low, other_half(one), two)


def col_setup_kernel(
    place_ref, raw_ref, ranks_ref, z_ref, own_ref, sent_ref, keep_ref, send_ref,
    raw, moved, ranks, z, values, in_sems, out_sems, small_sems,
):
    _, quads, cells, _ = moved.shape
    tiles = 4 * quads
    parts = in_sems.shape[0]
    step = cells // parts
    core, tile = place_ref[0], place_ref[1]

    def arrival(piece):
        rows = pl.ds(pl.multiple_of(piece * step * tiles, 16), step * tiles)
        return pltpu.make_async_copy(raw_ref.at[rows], raw.at[rows], in_sems.at[piece])

    def departures(piece):
        at = pl.ds(pl.multiple_of(piece * step, 16), step)
        return [
            pltpu.make_async_copy(
                moved.at[which, :, at, :], ref.at[:, at, :], out_sems.at[side, piece]
            )
            for side, (which, ref) in enumerate(((core, own_ref), (1 - core, sent_ref)))
        ]

    def launch(piece, carry):
        arrival(piece).start()
        return carry

    lax.fori_loop(0, parts, launch, 0)
    small = [
        pltpu.make_async_copy(z_ref, z, small_sems.at[0]),
        pltpu.make_async_copy(ranks_ref, ranks, small_sems.at[1]),
    ]
    for copy in small:
        copy.start()
    order = one_hot(tile_major)

    def turn(piece, carry):
        arrival(piece).wait()
        for group in range(step // 16):
            cell = pl.multiple_of(piece * step + group * 16, 16)
            blocks = read_blocks(raw, cell, tiles)
            for pair in range(2):
                one, two = blocks[2 * pair : 2 * pair + 2]
                both = jnp.concatenate(
                    [half_lanes(one, two, 0), half_lanes(one, two, 1)], axis=1
                )
                turned = jnp.dot(order, both, preferred_element_type=F32).astype(BF16)
                lanes = slice(pair * 128, pair * 128 + 128)
                for q in range(16):
                    for which in range(2):
                        moved[which, q, pl.ds(cell, 16), lanes] = turned[
                            q * 16 : (q + 1) * 16, which * 128 : which * 128 + 128
                        ]
        for copy in departures(piece):
            copy.start()
        return carry

    lax.fori_loop(0, parts, turn, 0)
    for copy in small:
        copy.wait()
    values[...] = z[...].astype(BF16)
    lane = lax.broadcasted_iota(jnp.int32, (8, 128), 1)
    low_lane = lane < 64
    for which, out_ref in ((1 - core, send_ref), (core, keep_ref)):
        level = lane % 64 + 64 * which

        def factor(q):
            return jnp.dot(values[...], moved[which, q], preferred_element_type=F32)

        def live(pair, q):
            one = q + 32 * pair
            top = jnp.where(low_lane, ranks[one, tile], ranks[one + 16, tile])
            return (level < top).astype(F32)[:1]

        project(factor, quads, live, out_ref)

    def finish(piece, carry):
        for copy in departures(piece):
            copy.wait()
        return carry

    lax.fori_loop(0, parts, finish, 0)


def col_setup(factors, place, tile_ranks, z, coefficients):
    cells, tiles, ranked = factors.shape
    shape = (tiles // 4, cells, 2 * ranked)
    parts = 8
    return pl.pallas_call(
        col_setup_kernel,
        in_specs=[SMEM, ANY, ANY, ANY],
        out_specs=[ANY] * 2 + [VMEM] * 2,
        out_shape=[pltpu.HBM(shape, BF16)] * 2 + [jax.ShapeDtypeStruct(*coefficients)] * 2,
        scratch_shapes=[
            pltpu.VMEM((cells * tiles, ranked), BF16),
            pltpu.VMEM((2, *shape), BF16),
            pltpu.SMEM(tile_ranks.shape, jnp.int32),
            pltpu.VMEM(z.shape, F32),
            pltpu.VMEM(z.shape, BF16),
            pltpu.SemaphoreType.DMA((parts,)),
            pltpu.SemaphoreType.DMA((2, parts)),
            pltpu.SemaphoreType.DMA((2,)),
        ],
        compiler_params=pltpu.CompilerParams(vmem_limit_bytes=24 << 20),
        cost_estimate=pl.CostEstimate(
            flops=8_000_000_000, bytes_accessed=1 << 24, transcendentals=0
        ),
    )(place, in_hbm(factors.reshape(cells * tiles, ranked)), in_hbm(tile_ranks), in_hbm(z))


def row_setup_kernel(place_ref, own_raw_ref, other_raw_ref, out_ref, raw, moved, in_sems, out_sems):
    _, quads, cells, _ = moved.shape
    tiles = 4 * quads
    parts = in_sems.shape[1]
    step = cells // parts
    order = one_hot(tile_major)

    def arrival(side, piece):
        rows = pl.ds(pl.multiple_of(piece * step * tiles, 16), step * tiles)
        source = (own_raw_ref, other_raw_ref)[side]
        return pltpu.make_async_copy(
            source.at[rows], raw.at[side, rows], in_sems.at[side, piece]
        )

    def departure(side, piece):
        at = pl.ds(pl.multiple_of(piece * step, 16), step)
        return pltpu.make_async_copy(
            moved.at[side, :, at, :], out_ref.at[side, :, at, :], out_sems.at[side, piece]
        )

    for side in range(2):
        def launch(piece, carry):
            arrival(side, piece).start()
            return carry

        lax.fori_loop(0, parts, launch, 0)
    for which in range(2):
        @pl.when(place_ref[0] == which)
        def _():
            for side in range(2):
                def turn(piece, carry):
                    arrival(side, piece).wait()
                    for group in range(step // 16):
                        cell = pl.multiple_of(piece * step + group * 16, 16)
                        blocks = read_blocks(raw.at[side], cell, tiles)
                        both = jnp.concatenate(
                            [
                                half_lanes(*blocks[2 * pair : 2 * pair + 2], which)
                                for pair in range(2)
                            ],
                            axis=1,
                        )
                        turned = jnp.dot(
                            order, both, preferred_element_type=F32
                        ).astype(BF16)
                        for q in range(16):
                            moved[side, q, pl.ds(cell, 16), :] = turned[
                                q * 16 : (q + 1) * 16
                            ]
                    departure(side, piece).start()
                    return carry

                lax.fori_loop(0, parts, turn, 0)

    for side in range(2):
        def finish(piece, carry):
            departure(side, piece).wait()
            return carry

        lax.fori_loop(0, parts, finish, 0)


def row_setup(own, other, place):
    cells, tiles, ranked = own.shape
    shape = (2, tiles // 4, cells, 2 * ranked)
    parts = 8
    rows = (cells * tiles, ranked)
    return pl.pallas_call(
        row_setup_kernel,
        in_specs=[SMEM, ANY, ANY],
        out_specs=ANY,
        out_shape=pltpu.HBM(shape, BF16),
        scratch_shapes=[
            pltpu.VMEM((2, *rows), BF16),
            pltpu.VMEM(shape, BF16),
            pltpu.SemaphoreType.DMA((2, parts)),
            pltpu.SemaphoreType.DMA((2, parts)),
        ],
        compiler_params=pltpu.CompilerParams(vmem_limit_bytes=32 << 20),
        cost_estimate=pl.CostEstimate(
            flops=8_000_000_000, bytes_accessed=1 << 24, transcendentals=0
        ),
    )(place, in_hbm(own.reshape(rows)), in_hbm(other.reshape(rows)))


def merge_kernel(after_ref, *refs):
    sources, (out_ref, turned_ref, sems) = refs[:-3], refs[-3:]
    if len(sources) == 1:
        sources = sources[0].at[0], sources[0].at[1]
    quads, cells = out_ref.shape[1], out_ref.shape[2]
    size = quads // sems.shape[1]
    same = one_hot(lambda to: to)

    def copies(group):
        quad = pl.ds(group * size, size)
        return [
            pltpu.make_async_copy(
                source.at[quad], out_ref.at[side, quad], sems.at[side, group]
            )
            for side, source in enumerate(sources)
        ]

    def launch(group, carry):
        for copy in copies(group):
            copy.start()
        return carry

    lax.fori_loop(0, sems.shape[1], launch, 0)

    def turn(group, carry):
        for copy in copies(group):
            copy.wait()
        for q in range(size):
            quad = group * size + q
            for side in range(2):
                for block in range(cells // 256):
                    at_cell = slice(256 * block, 256 * block + 256)
                    turned_ref[side, quad, :, at_cell] = lax.dot_general(
                        same, out_ref[side, quad, at_cell, :], NT,
                        preferred_element_type=F32,
                    ).astype(BF16)
        return carry

    lax.fori_loop(0, sems.shape[1], turn, 0)


def merge(after, *parts):
    quads, cells, lanes = parts[0].shape[-3:]
    return pl.pallas_call(
        merge_kernel,
        in_specs=[ANY] * (1 + len(parts)),
        out_specs=[VMEM] * 2,
        out_shape=[
            jax.ShapeDtypeStruct((2, quads, cells, lanes), BF16),
            jax.ShapeDtypeStruct((2, quads, lanes, cells), BF16),
        ],
        scratch_shapes=[pltpu.SemaphoreType.DMA((2, 8))],
        compiler_params=pltpu.CompilerParams(vmem_limit_bytes=4 << 20),
        cost_estimate=pl.CostEstimate(
            flops=4_000_000_000, bytes_accessed=1 << 24, transcendentals=0
        ),
    )(after, *[in_hbm(part) for part in parts])


def add_kernel(keep_ref, arrived_ref, out_ref):
    out_ref[...] = (keep_ref[...].astype(F32) + arrived_ref[...].astype(F32)).astype(BF16)


def expand_kernel(coefficient_ref, turned_ref, total_ref, left):
    quads, cells = turned_ref.shape[1], turned_ref.shape[3]
    half = coefficient_ref.shape[1]

    def arrange(q, carry):
        for pair in range(2):
            one = coefficient_ref[q + 32 * pair]
            two = coefficient_ref[q + 32 * pair + 16]
            low = low_lanes(one)
            lanes = slice(pair * 128, pair * 128 + 128)
            left[q, :half, lanes] = jnp.where(low, one, other_half(two))
            left[q, half:, lanes] = jnp.where(low, other_half(one), two)
        return carry

    lax.fori_loop(0, quads, arrange, 0, unroll=4)

    def side_of(side, carry):
        for block in range(cells // 256):
            at_cell = slice(256 * block, 256 * block + 256)
            at = pl.ds(pl.multiple_of(side * cells + 256 * block, 256), 256)
            total_ref[:, at] = sum(
                jnp.dot(
                    left[q], turned_ref[side, q, :, at_cell], preferred_element_type=F32
                )
                for q in range(quads)
            )
        return carry

    lax.fori_loop(0, 2, side_of, 0)


def project(factor, quads, live, out_ref):
    half = out_ref.shape[1]
    low = lax.broadcasted_iota(jnp.int32, (half, 128), 1) < 64

    def quad(q, carry):
        moved = factor(q)
        for pair in range(2):
            one, two = q + 32 * pair, q + 32 * pair + 16
            part = moved[:, pair * 128 : pair * 128 + 128] * live(pair, q)
            part = part.astype(BF16)
            turned = other_half(part)
            out_ref[one] = jnp.where(low, part[:half], turned[half:])
            out_ref[two] = jnp.where(low, turned[:half], part[half:])
        return carry

    lax.fori_loop(0, quads, quad, 0, unroll=UNROLL)


def project_both(values, f_ref, live_ref, out_ref):
    cells = f_ref.shape[2]

    def factor(q):
        return jnp.dot(
            values[:, :cells], f_ref[0, q], preferred_element_type=F32
        ) + jnp.dot(values[:, cells:], f_ref[1, q], preferred_element_type=F32)

    def live(pair, q):
        return live_ref[pair * 16 + q, :1]

    project(factor, f_ref.shape[1], live, out_ref)


def complete(total_ref, arrived_ref):
    cells = total_ref.shape[1] // 2
    return [
        total_ref[:, :cells] + arrived_ref[:, cells:],
        total_ref[:, cells:] + arrived_ref[:, :cells],
    ]


def row_kernel(
    live_ref, total_ref, arrived_ref, base_ref, rate_ref, f_ref,
    out_ref, *refs,
):
    *energy_ref, values = refs
    cells = total_ref.shape[1] // 2
    for side, field in enumerate(complete(total_ref, arrived_ref)):
        at = slice(side * cells, (side + 1) * cells)
        rate = rate_ref[:, at]
        exponent = base_ref[:, at] + field
        intensity = jnp.exp(exponent)
        values[:, at] = (rate - intensity).astype(BF16)
        if side == 0 and energy_ref:
            energy_ref[0][...] = jnp.sum(intensity - rate * exponent, axis=1, keepdims=True)
    project_both(values, f_ref, live_ref, out_ref)


def col_kernel(
    weight, live_ref, total_ref, arrived_ref, step_ref, z_ref, m_ref,
    f_ref, out_ref, new_z_ref, new_m_ref, values,
):
    cells = total_ref.shape[1] // 2
    step = step_ref[:, :1]
    for side, pulled in enumerate(complete(total_ref, arrived_ref)):
        at = slice(side * cells, (side + 1) * cells)
        z = z_ref[:, at]
        moment = m_ref[:, at] - weight * step * (z - pulled)
        z = z + step * moment
        new_m_ref[:, at] = moment
        new_z_ref[:, at] = z
        values[:, at] = z.astype(BF16)
    project_both(values, f_ref, live_ref, out_ref)


def last_kernel(
    total_ref, arrived_ref, step_ref, z_ref, m_ref, start_z_ref, start_m_ref,
    start_energy_ref, end_energy_ref, new_m_ref, change_ref,
):
    cells = total_ref.shape[1] // 2
    z = z_ref[:, :cells]
    moment = m_ref[:, :cells] - 0.5 * step_ref[:, :1] * (
        z - complete(total_ref, arrived_ref)[0]
    )
    new_m_ref[...] = moment
    start_z = start_z_ref[:, :cells]
    start_m = start_m_ref[:, :cells]
    pieces = 0.5 * (z * z - start_z * start_z + moment * moment - start_m * start_m)
    change = (
        jnp.sum(pieces, axis=1, keepdims=True) + end_energy_ref[...] - start_energy_ref[...]
    )
    row = jnp.transpose(jnp.broadcast_to(change, (change.shape[0], change.shape[0])))[:1]
    change_ref[...] = jnp.broadcast_to(row[None], change_ref.shape)


def call(kernel, specs, outs, scratch, flops, *args):
    return pl.pallas_call(
        kernel,
        in_specs=specs,
        out_specs=[VMEM] * len(outs),
        out_shape=[jax.ShapeDtypeStruct(*o) for o in outs],
        scratch_shapes=scratch,
        compiler_params=pltpu.CompilerParams(vmem_limit_bytes=LIMIT),
        cost_estimate=pl.CostEstimate(
            flops=flops, bytes_accessed=1 << 24, transcendentals=0
        ),
    )(*args)


def on_device(
    position, momentum, row_factors, col_factors, tile_ranks, log_mean, counts, step_size
):
    chains, cells = position.shape
    half = chains // 2
    tiles, ranked = tile_ranks.shape[0], row_factors.shape[2]
    tile = lax.axis_index(CHIPS)
    core = lax.axis_index(CORE).astype(jnp.int32)
    place = jnp.stack([core, tile.astype(jnp.int32)])
    lane = jnp.arange(ranked, dtype=jnp.int32)

    def live(ranks):
        tops = ranks.reshape(2, 2, tiles // 4)
        top = jnp.where(lane < ranked // 2, tops[:, 0, :, None], tops[:, 1, :, None])
        level = lane % (ranked // 2) + ranked // 2 * core
        alive = (level < top).astype(F32).reshape(tiles // 2, 1, ranked)
        return jnp.broadcast_to(alive, (tiles // 2, 8, ranked))

    coefficients = ((tiles, half, ranked), BF16)
    state = ((chains, 2 * cells), F32)
    own_state = ((chains, cells), F32)
    column = ((chains, 1), F32)
    values = [pltpu.VMEM((chains, 2 * cells), BF16)]
    left = [pltpu.VMEM((tiles // 4, chains, 2 * ranked), BF16)]
    work = 2 * chains * 2 * cells * tiles * ranked // 2

    row_arrived = swap(row_factors)
    col_own, col_sent, keep, send = col_setup(
        col_factors, place, tile_ranks, position, coefficients
    )
    (out,) = call(add_kernel, [VMEM] * 2, [coefficients], [], 1 << 24, keep, swap(send))
    out, col_sent, row_factors, row_arrived, late = lax.optimization_barrier(
        (
            out, col_sent, row_factors, row_arrived,
            (position, momentum, tile_ranks, log_mean, counts, step_size),
        )
    )
    arrived = spread(out)
    position, momentum, tile_ranks, log_mean, counts, step_size = late
    row_whole = row_setup(row_factors, row_arrived, place)
    rate = counts.astype(F32)
    z_other, m_other = swap(position), swap(momentum)
    base_other, rate_other = swap(log_mean), swap(rate)
    col_other = swap(col_sent)
    col_live = live(lax.dynamic_slice_in_dim(tile_ranks, tile, 1, 1)[:, 0])
    row_live = live(lax.dynamic_slice_in_dim(tile_ranks, tile, 1, 0)[0])
    start_z = jnp.concatenate([position, z_other], axis=1)
    start_m = jnp.concatenate([momentum, m_other], axis=1)
    base = jnp.concatenate([log_mean, base_other])[None, :]
    rate = jnp.concatenate([rate, rate_other])[None, :]
    step = jnp.broadcast_to(step_size[:, None], (chains, ranked))

    def expand(coefficient, factors):
        (total,) = call(
            expand_kernel, [VMEM] * 2, [state], left, 2 * work, coefficient, factors[1]
        )
        return total, swap(total)

    def row_pass(arrived, energy=True):
        return call(
            row_kernel, [VMEM] * 6, [coefficients] + [column] * energy, values, work,
            row_live, *expand(arrived, row), base, rate, row[0],
        )

    arrived, start_z, start_m, base, rate, step, row_live, col_live = (
        lax.optimization_barrier(
            (arrived, start_z, start_m, base, rate, step, row_live, col_live)
        )
    )
    z, m = start_z, start_m
    row = merge(arrived, row_whole)
    out, start_energy = row_pass(arrived)
    out, col_other = lax.optimization_barrier((out, col_other))
    arrived = spread(out)
    col = merge(arrived, col_own, col_other)
    for weight in (0.5, 1.0):
        out, z, m = call(
            functools.partial(col_kernel, weight),
            [VMEM] * 7, [coefficients, state, state], values, work,
            col_live, *expand(arrived, col), step, z, m, col[0],
        )
        last = weight == 1.0
        out, *energy = row_pass(spread(out), last)
        arrived = spread(out)
    (end_energy,) = energy
    m, change = call(
        last_kernel, [VMEM] * 9, [own_state, ((tiles, 1, chains), F32)], [], 1 << 24,
        *expand(arrived, col), step, z, m, start_z, start_m,
        start_energy, end_energy,
    )
    change = spread(change)
    z = z[:, :cells]
    change = change.sum(axis=(0, 1))
    change = change + swap(change)
    return z, m, change


def solution(mesh):
    split = Mesh(
        mesh.devices.reshape(4, 4, 4, 2), ("col_0", "col_1", "row_0", "row_1")
    )
    return jax.shard_map(
        on_device,
        mesh=split,
        in_specs=(
            P(None, COL_ROW),
            P(None, COL_ROW),
            P(COL_ROW, None, None),
            P(COL_ROW, None, None),
            P(),
            P(COL_ROW),
            P(COL_ROW),
            P(),
        ),
        out_specs=(P(None, COL_ROW), P(None, COL_ROW), P()),
        check_vma=False,
    )
```

```python
import functools

import jax
import jax.numpy as jnp
from jax import lax
from jax.experimental import pallas as pl
from jax.experimental.pallas import tpu as pltpu
from jax.sharding import Mesh
from jax.sharding import PartitionSpec as P

COL_ROW = ("col_0", "col_1", "row_0", "row_1")
CHIPS = ("col_0", "col_1", "row_0")
CORE = "row_1"
BF16 = jnp.bfloat16
F32 = jnp.float32
LIMIT = 8 << 20
UNROLL = 8
VMEM = pl.BlockSpec(memory_space=pltpu.VMEM)
SMEM = pl.BlockSpec(memory_space=pltpu.SMEM)
ANY = pl.BlockSpec(memory_space=pl.ANY)


def swap(value):
    return lax.ppermute(value, CORE, [(0, 1), (1, 0)])


def spread(value):
    return lax.all_to_all(value, CHIPS, split_axis=0, concat_axis=0, tiled=True)


def in_hbm(value):
    return pltpu.with_memory_space_constraint(value, pltpu.HBM)


def other_half(value):
    lanes = value.shape[1] // 2
    return jnp.concatenate([value[:, lanes:], value[:, :lanes]], axis=1)


def low_lanes(value):
    return lax.broadcasted_iota(jnp.int32, value.shape, 1) < value.shape[1] // 2


def one_hot(index):
    to = lax.broadcasted_iota(jnp.int32, (256, 256), 0)
    at = lax.broadcasted_iota(jnp.int32, (256, 256), 1)
    return (at == index(to)).astype(F32).astype(BF16)


def tile_major(to):
    return (to % 16) * 16 + to // 16


def read_blocks(raw, cell, tiles):
    return [
        jnp.concatenate(
            [
                raw[pl.ds(pl.multiple_of((cell + y) * tiles + block * 16, 16), 16), :]
                for y in range(16)
            ],
            axis=0,
        )
        for block in range(tiles // 16)
    ]


def half_lanes(one, two, which):
    low = low_lanes(one)
    if which == 0:
        return jnp.where(low, one, other_half(two))
    return jnp.where(low, other_half(one), two)


def col_setup_kernel(
    place_ref, raw_ref, ranks_ref, z_ref, own_ref, sent_ref, keep_ref, send_ref,
    raw, moved, ranks, z, values, in_sems, out_sems, small_sems,
):
    _, quads, cells, _ = moved.shape
    tiles = 4 * quads
    parts = in_sems.shape[0]
    step = cells // parts
    core, tile = place_ref[0], place_ref[1]

    def arrival(piece):
        rows = pl.ds(pl.multiple_of(piece * step * tiles, 16), step * tiles)
        return pltpu.make_async_copy(raw_ref.at[rows], raw.at[rows], in_sems.at[piece])

    def departures(piece):
        at = pl.ds(pl.multiple_of(piece * step, 16), step)
        return [
            pltpu.make_async_copy(
                moved.at[which, :, at, :], ref.at[:, at, :], out_sems.at[side, piece]
            )
            for side, (which, ref) in enumerate(((core, own_ref), (1 - core, sent_ref)))
        ]

    def launch(piece, carry):
        arrival(piece).start()
        return carry

    lax.fori_loop(0, parts, launch, 0)
    small = [
        pltpu.make_async_copy(z_ref, z, small_sems.at[0]),
        pltpu.make_async_copy(ranks_ref, ranks, small_sems.at[1]),
    ]
    for copy in small:
        copy.start()
    order = one_hot(tile_major)

    def turn(piece, carry):
        arrival(piece).wait()
        for group in range(step // 16):
            cell = pl.multiple_of(piece * step + group * 16, 16)
            blocks = read_blocks(raw, cell, tiles)
            for pair in range(2):
                one, two = blocks[2 * pair : 2 * pair + 2]
                both = jnp.concatenate(
                    [half_lanes(one, two, 0), half_lanes(one, two, 1)], axis=1
                )
                turned = jnp.dot(order, both, preferred_element_type=F32).astype(BF16)
                lanes = slice(pair * 128, pair * 128 + 128)
                for q in range(16):
                    for which in range(2):
                        moved[which, q, pl.ds(cell, 16), lanes] = turned[
                            q * 16 : (q + 1) * 16, which * 128 : which * 128 + 128
                        ]
        for copy in departures(piece):
            copy.start()
        return carry

    lax.fori_loop(0, parts, turn, 0)
    for copy in small:
        copy.wait()
    values[...] = z[...].astype(BF16)
    lane = lax.broadcasted_iota(jnp.int32, (8, 128), 1)
    low_lane = lane < 64
    for which, out_ref in ((1 - core, send_ref), (core, keep_ref)):
        level = lane % 64 + 64 * which

        def factor(q):
            return jnp.dot(values[...], moved[which, q], preferred_element_type=F32)

        def live(pair, q):
            one = q + 32 * pair
            top = jnp.where(low_lane, ranks[one, tile], ranks[one + 16, tile])
            return (level < top).astype(F32)[:1]

        project(factor, quads, live, out_ref)

    def finish(piece, carry):
        for copy in departures(piece):
            copy.wait()
        return carry

    lax.fori_loop(0, parts, finish, 0)


def col_setup(factors, place, tile_ranks, z, coefficients):
    cells, tiles, ranked = factors.shape
    shape = (tiles // 4, cells, 2 * ranked)
    parts = 8
    return pl.pallas_call(
        col_setup_kernel,
        in_specs=[SMEM, ANY, ANY, ANY],
        out_specs=[ANY] * 2 + [VMEM] * 2,
        out_shape=[pltpu.HBM(shape, BF16)] * 2 + [jax.ShapeDtypeStruct(*coefficients)] * 2,
        scratch_shapes=[
            pltpu.VMEM((cells * tiles, ranked), BF16),
            pltpu.VMEM((2, *shape), BF16),
            pltpu.SMEM(tile_ranks.shape, jnp.int32),
            pltpu.VMEM(z.shape, F32),
            pltpu.VMEM(z.shape, BF16),
            pltpu.SemaphoreType.DMA((parts,)),
            pltpu.SemaphoreType.DMA((2, parts)),
            pltpu.SemaphoreType.DMA((2,)),
        ],
        compiler_params=pltpu.CompilerParams(vmem_limit_bytes=24 << 20),
        cost_estimate=pl.CostEstimate(
            flops=8_000_000_000, bytes_accessed=1 << 24, transcendentals=0
        ),
    )(place, in_hbm(factors.reshape(cells * tiles, ranked)), in_hbm(tile_ranks), in_hbm(z))


def row_setup_kernel(place_ref, own_raw_ref, other_raw_ref, out_ref, raw, moved, in_sems, out_sems):
    _, quads, cells, _ = moved.shape
    tiles = 4 * quads
    parts = in_sems.shape[1]
    step = cells // parts
    order = one_hot(tile_major)

    def arrival(side, piece):
        rows = pl.ds(pl.multiple_of(piece * step * tiles, 16), step * tiles)
        source = (own_raw_ref, other_raw_ref)[side]
        return pltpu.make_async_copy(
            source.at[rows], raw.at[side, rows], in_sems.at[side, piece]
        )

    def departure(side, piece):
        at = pl.ds(pl.multiple_of(piece * step, 16), step)
        return pltpu.make_async_copy(
            moved.at[side, :, at, :], out_ref.at[side, :, at, :], out_sems.at[side, piece]
        )

    for side in range(2):
        def launch(piece, carry):
            arrival(side, piece).start()
            return carry

        lax.fori_loop(0, parts, launch, 0)
    for which in range(2):
        @pl.when(place_ref[0] == which)
        def _():
            for side in range(2):
                def turn(piece, carry):
                    arrival(side, piece).wait()
                    for group in range(step // 16):
                        cell = pl.multiple_of(piece * step + group * 16, 16)
                        blocks = read_blocks(raw.at[side], cell, tiles)
                        both = jnp.concatenate(
                            [
                                half_lanes(*blocks[2 * pair : 2 * pair + 2], which)
                                for pair in range(2)
                            ],
                            axis=1,
                        )
                        turned = jnp.dot(
                            order, both, preferred_element_type=F32
                        ).astype(BF16)
                        for q in range(16):
                            moved[side, q, pl.ds(cell, 16), :] = turned[
                                q * 16 : (q + 1) * 16
                            ]
                    departure(side, piece).start()
                    return carry

                lax.fori_loop(0, parts, turn, 0)

    for side in range(2):
        def finish(piece, carry):
            departure(side, piece).wait()
            return carry

        lax.fori_loop(0, parts, finish, 0)


def row_setup(own, other, place):
    cells, tiles, ranked = own.shape
    shape = (2, tiles // 4, cells, 2 * ranked)
    parts = 8
    rows = (cells * tiles, ranked)
    return pl.pallas_call(
        row_setup_kernel,
        in_specs=[SMEM, ANY, ANY],
        out_specs=ANY,
        out_shape=pltpu.HBM(shape, BF16),
        scratch_shapes=[
            pltpu.VMEM((2, *rows), BF16),
            pltpu.VMEM(shape, BF16),
            pltpu.SemaphoreType.DMA((2, parts)),
            pltpu.SemaphoreType.DMA((2, parts)),
        ],
        compiler_params=pltpu.CompilerParams(vmem_limit_bytes=32 << 20),
        cost_estimate=pl.CostEstimate(
            flops=8_000_000_000, bytes_accessed=1 << 24, transcendentals=0
        ),
    )(place, in_hbm(own.reshape(rows)), in_hbm(other.reshape(rows)))


def merge_kernel(after_ref, *refs):
    sources, (out_ref, turned_ref, sems) = refs[:-3], refs[-3:]
    if len(sources) == 1:
        sources = sources[0].at[0], sources[0].at[1]
    quads, cells = out_ref.shape[1], out_ref.shape[2]
    size = quads // sems.shape[1]

    def copies(group):
        quad = pl.ds(group * size, size)
        return [
            pltpu.make_async_copy(
                source.at[quad], out_ref.at[side, quad], sems.at[side, group]
            )
            for side, source in enumerate(sources)
        ]

    def launch(group, carry):
        for copy in copies(group):
            copy.start()
        return carry

    lax.fori_loop(0, sems.shape[1], launch, 0)

    def turn(group, carry):
        for copy in copies(group):
            copy.wait()
        for q in range(size):
            quad = group * size + q
            for side in range(2):
                for block in range(cells // 256):
                    at_cell = slice(256 * block, 256 * block + 256)
                    turned_ref[side, quad, :, at_cell] = jnp.transpose(
                        out_ref[side, quad, at_cell, :]
                    )
        return carry

    lax.fori_loop(0, sems.shape[1], turn, 0)


def merge(after, *parts):
    quads, cells, lanes = parts[0].shape[-3:]
    return pl.pallas_call(
        merge_kernel,
        in_specs=[ANY] * (1 + len(parts)),
        out_specs=[VMEM] * 2,
        out_shape=[
            jax.ShapeDtypeStruct((2, quads, cells, lanes), BF16),
            jax.ShapeDtypeStruct((2, quads, lanes, cells), BF16),
        ],
        scratch_shapes=[pltpu.SemaphoreType.DMA((2, 8))],
        compiler_params=pltpu.CompilerParams(vmem_limit_bytes=4 << 20),
        cost_estimate=pl.CostEstimate(
            flops=4_000_000_000, bytes_accessed=1 << 24, transcendentals=0
        ),
    )(after, *[in_hbm(part) for part in parts])


def add_kernel(keep_ref, arrived_ref, out_ref):
    out_ref[...] = (keep_ref[...].astype(F32) + arrived_ref[...].astype(F32)).astype(BF16)


def expand_side(side, left_ref, turned_ref, total_ref):
    quads, cells = turned_ref.shape[1], turned_ref.shape[3]
    for block in range(cells // 256):
        at_cell = slice(256 * block, 256 * block + 256)
        total_ref[:, at_cell] = sum(
            jnp.dot(
                left_ref[q], turned_ref[side, q, :, at_cell], preferred_element_type=F32
            )
            for q in range(quads)
        )


def expand_first_kernel(side, coefficient_ref, turned_ref, total_ref, left_ref):
    half = coefficient_ref.shape[1]

    def arrange(q, carry):
        for pair in range(2):
            one = coefficient_ref[q + 32 * pair]
            two = coefficient_ref[q + 32 * pair + 16]
            low = low_lanes(one)
            lanes = slice(pair * 128, pair * 128 + 128)
            left_ref[q, :half, lanes] = jnp.where(low, one, other_half(two))
            left_ref[q, half:, lanes] = jnp.where(low, other_half(one), two)
        return carry

    lax.fori_loop(0, left_ref.shape[0], arrange, 0, unroll=4)
    expand_side(side, left_ref, turned_ref, total_ref)


def project(factor, quads, live, out_ref):
    half = out_ref.shape[1]
    low = lax.broadcasted_iota(jnp.int32, (half, 128), 1) < 64

    def quad(q, carry):
        moved = factor(q)
        for pair in range(2):
            one, two = q + 32 * pair, q + 32 * pair + 16
            part = moved[:, pair * 128 : pair * 128 + 128] * live(pair, q)
            part = part.astype(BF16)
            turned = other_half(part)
            out_ref[one] = jnp.where(low, part[:half], turned[half:])
            out_ref[two] = jnp.where(low, turned[:half], part[half:])
        return carry

    lax.fori_loop(0, quads, quad, 0, unroll=UNROLL)


def row_values(total_ref, arrived_ref, base_ref, rate_ref, values):
    rate = rate_ref[...]
    exponent = base_ref[...] + (total_ref[...] + arrived_ref[...])
    intensity = jnp.exp(exponent)
    values[...] = (rate - intensity).astype(BF16)
    return intensity - rate * exponent


def col_values(
    weight, total_ref, arrived_ref, step_ref, z_ref, m_ref, new_z_ref, new_m_ref, values
):
    step = step_ref[:, :1]
    z = z_ref[...]
    moment = m_ref[...] - weight * step * (z - (total_ref[...] + arrived_ref[...]))
    z = z + step * moment
    new_m_ref[...] = moment
    new_z_ref[...] = z
    values[...] = z.astype(BF16)


def project_first(values, f_ref, part_ref):
    def quad(q, carry):
        part_ref[q] = jnp.dot(values[...], f_ref[1, q], preferred_element_type=F32)
        return carry

    lax.fori_loop(0, part_ref.shape[0], quad, 0, unroll=UNROLL)


def project_second(values, f_ref, part_ref, live_ref, out_ref):
    def factor(q):
        return part_ref[q] + jnp.dot(
            values[...], f_ref[0, q], preferred_element_type=F32
        )

    def live(pair, q):
        return live_ref[pair * 16 + q, :1]

    project(factor, part_ref.shape[0], live, out_ref)


def row_first_kernel(total_ref, arrived_ref, base_ref, rate_ref, f_ref, part_ref, values):
    row_values(total_ref, arrived_ref, base_ref, rate_ref, values)
    project_first(values, f_ref, part_ref)


def row_second_kernel(
    live_ref, total_ref, arrived_ref, base_ref, rate_ref, f_ref, part_ref, out_ref, *refs
):
    *energy_ref, values = refs
    energy = row_values(total_ref, arrived_ref, base_ref, rate_ref, values)
    if energy_ref:
        energy_ref[0][...] = jnp.sum(energy, axis=1, keepdims=True)
    project_second(values, f_ref, part_ref, live_ref, out_ref)


def col_first_kernel(
    weight, total_ref, arrived_ref, step_ref, z_ref, m_ref, f_ref,
    part_ref, new_z_ref, new_m_ref, values,
):
    col_values(
        weight, total_ref, arrived_ref, step_ref, z_ref, m_ref, new_z_ref, new_m_ref, values
    )
    project_first(values, f_ref, part_ref)


def col_second_kernel(
    weight, live_ref, total_ref, arrived_ref, step_ref, z_ref, m_ref, f_ref, part_ref,
    out_ref, new_z_ref, new_m_ref, values,
):
    col_values(
        weight, total_ref, arrived_ref, step_ref, z_ref, m_ref, new_z_ref, new_m_ref, values
    )
    project_second(values, f_ref, part_ref, live_ref, out_ref)


def last_kernel(
    total_ref, arrived_ref, step_ref, z_ref, m_ref, start_z_ref, start_m_ref,
    start_energy_ref, end_energy_ref, new_m_ref, change_ref,
):
    z = z_ref[...]
    moment = m_ref[...] - 0.5 * step_ref[:, :1] * (
        z - (total_ref[...] + arrived_ref[...])
    )
    new_m_ref[...] = moment
    start_z = start_z_ref[...]
    start_m = start_m_ref[...]
    pieces = 0.5 * (z * z - start_z * start_z + moment * moment - start_m * start_m)
    change = (
        jnp.sum(pieces, axis=1, keepdims=True) + end_energy_ref[...] - start_energy_ref[...]
    )
    row = jnp.transpose(jnp.broadcast_to(change, (change.shape[0], change.shape[0])))[:1]
    change_ref[...] = jnp.broadcast_to(row[None], change_ref.shape)


def call(kernel, specs, outs, scratch, flops, *args):
    return pl.pallas_call(
        kernel,
        in_specs=specs,
        out_specs=[VMEM] * len(outs),
        out_shape=[jax.ShapeDtypeStruct(*o) for o in outs],
        scratch_shapes=scratch,
        compiler_params=pltpu.CompilerParams(vmem_limit_bytes=LIMIT),
        cost_estimate=pl.CostEstimate(
            flops=flops, bytes_accessed=1 << 24, transcendentals=0
        ),
    )(*args)


def on_device(
    position, momentum, row_factors, col_factors, tile_ranks, log_mean, counts, step_size
):
    chains, cells = position.shape
    half = chains // 2
    tiles, ranked = tile_ranks.shape[0], row_factors.shape[2]
    tile = lax.axis_index(CHIPS)
    core = lax.axis_index(CORE).astype(jnp.int32)
    place = jnp.stack([core, tile.astype(jnp.int32)])
    lane = jnp.arange(ranked, dtype=jnp.int32)

    def live(ranks):
        tops = ranks.reshape(2, 2, tiles // 4)
        top = jnp.where(lane < ranked // 2, tops[:, 0, :, None], tops[:, 1, :, None])
        level = lane % (ranked // 2) + ranked // 2 * core
        alive = (level < top).astype(F32).reshape(tiles // 2, 1, ranked)
        return jnp.broadcast_to(alive, (tiles // 2, 8, ranked))

    coefficients = ((tiles, half, ranked), BF16)
    state = ((chains, cells), F32)
    part = ((tiles // 4, chains, 2 * ranked), F32)
    left = ((tiles // 4, chains, 2 * ranked), BF16)
    column = ((chains, 1), F32)
    values = [pltpu.VMEM((chains, cells), BF16)]
    work = 2 * chains * cells * tiles * ranked // 2

    row_arrived = swap(row_factors)
    col_own, col_sent, keep, send = col_setup(
        col_factors, place, tile_ranks, position, coefficients
    )
    sent = swap(send)
    (out,) = call(add_kernel, [VMEM] * 2, [coefficients], [], 1 << 24, keep, sent)
    out, col_sent, row_factors, late = lax.optimization_barrier(
        (
            out, col_sent, row_factors,
            (position, momentum, tile_ranks, log_mean, counts, step_size),
        )
    )
    arrived = spread(out)
    position, momentum, tile_ranks, log_mean, counts, step_size = late
    row_whole = row_setup(row_factors, row_arrived, place)
    rate = counts.astype(F32)
    z_other, m_other = swap(position), swap(momentum)
    base_other, rate_other = swap(log_mean), swap(rate)
    col_other = swap(col_sent)
    col_live = live(lax.dynamic_slice_in_dim(tile_ranks, tile, 1, 1)[:, 0])
    row_live = live(lax.dynamic_slice_in_dim(tile_ranks, tile, 1, 0)[0])
    base = log_mean[None, :], base_other[None, :]
    rate = rate[None, :], rate_other[None, :]
    step = jnp.broadcast_to(step_size[:, None], (chains, ranked))

    def expand(coefficient, factors, first):
        one, rows = call(
            functools.partial(expand_first_kernel, first), [VMEM] * 2, [state, left], [],
            2 * work, coefficient, factors[1],
        )
        one_arrived = swap(one)
        (two,) = call(
            functools.partial(expand_side, 1 - first), [VMEM] * 2, [state], [],
            2 * work, rows, factors[1],
        )
        return one, two, one_arrived

    def row_pass(arrived, energy=True):
        own, other, for_other = expand(arrived, row, 0)
        for_own = swap(other)
        (share,) = call(
            row_first_kernel, [VMEM] * 5, [part], values, work,
            other, for_other, base[1], rate[1], row[0],
        )
        return call(
            row_second_kernel, [VMEM] * 7, [coefficients] + [column] * energy, values, work,
            row_live, own, for_own, base[0], rate[0], row[0], share,
        )

    def col_pass(weight, arrived, z, m):
        own, other, for_other = expand(arrived, col, 0)
        for_own = swap(other)
        share, z_partner, m_partner = call(
            functools.partial(col_first_kernel, weight), [VMEM] * 6, [part, state, state],
            values, work, other, for_other, step, z[1], m[1], col[0],
        )
        out, z_here, m_here = call(
            functools.partial(col_second_kernel, weight), [VMEM] * 8,
            [coefficients, state, state], values, work,
            col_live, own, for_own, step, z[0], m[0], col[0], share,
        )
        return out, (z_here, z_partner), (m_here, m_partner)

    arrived, position, momentum, z_other, m_other, base, rate, step, row_live, col_live = (
        lax.optimization_barrier(
            (
                arrived, position, momentum, z_other, m_other,
                base, rate, step, row_live, col_live,
            )
        )
    )
    z, m = (position, z_other), (momentum, m_other)
    row = merge(arrived, row_whole)
    out, start_energy = row_pass(arrived)
    out, col_other = lax.optimization_barrier((out, col_other))
    arrived = spread(out)
    col = merge(arrived, col_own, col_other)
    out, z, m = col_pass(0.5, arrived, z, m)
    (out,) = row_pass(spread(out), False)
    out, z, m = col_pass(1.0, spread(out), z, m)
    out, end_energy = row_pass(spread(out))
    _, own, for_own = expand(spread(out), col, 1)
    m, change = call(
        last_kernel, [VMEM] * 9, [state, ((tiles, 1, chains), F32)], [], 1 << 24,
        own, for_own, step, z[0], m[0], position, momentum, start_energy, end_energy,
    )
    change = spread(change)
    change = change.sum(axis=(0, 1))
    change = change + swap(change)
    return z[0], m, change


def solution(mesh):
    split = Mesh(
        mesh.devices.reshape(4, 4, 4, 2), ("col_0", "col_1", "row_0", "row_1")
    )
    return jax.shard_map(
        on_device,
        mesh=split,
        in_specs=(
            P(None, COL_ROW),
            P(None, COL_ROW),
            P(COL_ROW, None, None),
            P(COL_ROW, None, None),
            P(),
            P(COL_ROW),
            P(COL_ROW),
            P(),
        ),
        out_specs=(P(None, COL_ROW), P(None, COL_ROW), P()),
        check_vma=False,
    )
```

```python
import functools

import jax
import jax.numpy as jnp
from jax import lax
from jax.experimental import pallas as pl
from jax.experimental.pallas import tpu as pltpu
from jax.sharding import Mesh
from jax.sharding import PartitionSpec as P

COL_ROW = ("col_0", "col_1", "row_0", "row_1")
CHIPS = ("col_0", "col_1", "row_0")
CORE = "row_1"
BF16 = jnp.bfloat16
F32 = jnp.float32
LIMIT = 8 << 20
UNROLL = 8
VMEM = pl.BlockSpec(memory_space=pltpu.VMEM)
SMEM = pl.BlockSpec(memory_space=pltpu.SMEM)
ANY = pl.BlockSpec(memory_space=pl.ANY)


def swap(value):
    return lax.ppermute(value, CORE, [(0, 1), (1, 0)])


def spread(value):
    return lax.all_to_all(value, CHIPS, split_axis=0, concat_axis=0, tiled=True)


def in_hbm(value):
    return pltpu.with_memory_space_constraint(value, pltpu.HBM)


def other_half(value):
    lanes = value.shape[1] // 2
    return jnp.concatenate([value[:, lanes:], value[:, :lanes]], axis=1)


def low_lanes(value):
    return lax.broadcasted_iota(jnp.int32, value.shape, 1) < value.shape[1] // 2


def one_hot(index):
    to = lax.broadcasted_iota(jnp.int32, (256, 256), 0)
    at = lax.broadcasted_iota(jnp.int32, (256, 256), 1)
    return (at == index(to)).astype(F32).astype(BF16)


def tile_major(to):
    return (to % 16) * 16 + to // 16


def read_blocks(raw, cell, tiles):
    return [
        jnp.concatenate(
            [
                raw[pl.ds(pl.multiple_of((cell + y) * tiles + block * 16, 16), 16), :]
                for y in range(16)
            ],
            axis=0,
        )
        for block in range(tiles // 16)
    ]


def half_lanes(one, two, which):
    low = low_lanes(one)
    if which == 0:
        return jnp.where(low, one, other_half(two))
    return jnp.where(low, other_half(one), two)


def col_setup_kernel(
    place_ref, raw_ref, ranks_ref, z_ref, own_ref, sent_ref, keep_ref, send_ref,
    raw, moved, ranks, z, values, in_sems, out_sems, small_sems,
):
    _, quads, cells, _ = moved.shape
    tiles = 4 * quads
    parts = in_sems.shape[0]
    step = cells // parts
    core, tile = place_ref[0], place_ref[1]

    def arrival(piece):
        rows = pl.ds(pl.multiple_of(piece * step * tiles, 16), step * tiles)
        return pltpu.make_async_copy(raw_ref.at[rows], raw.at[rows], in_sems.at[piece])

    def departures(piece):
        at = pl.ds(pl.multiple_of(piece * step, 16), step)
        return [
            pltpu.make_async_copy(
                moved.at[which, :, at, :], ref.at[:, at, :], out_sems.at[side, piece]
            )
            for side, (which, ref) in enumerate(((core, own_ref), (1 - core, sent_ref)))
        ]

    def launch(piece, carry):
        arrival(piece).start()
        return carry

    lax.fori_loop(0, parts, launch, 0)
    small = [
        pltpu.make_async_copy(z_ref, z, small_sems.at[0]),
        pltpu.make_async_copy(ranks_ref, ranks, small_sems.at[1]),
    ]
    for copy in small:
        copy.start()
    order = one_hot(tile_major)

    def turn(piece, carry):
        arrival(piece).wait()
        for group in range(step // 16):
            cell = pl.multiple_of(piece * step + group * 16, 16)
            blocks = read_blocks(raw, cell, tiles)
            for pair in range(2):
                one, two = blocks[2 * pair : 2 * pair + 2]
                both = jnp.concatenate(
                    [half_lanes(one, two, 0), half_lanes(one, two, 1)], axis=1
                )
                turned = jnp.dot(order, both, preferred_element_type=F32).astype(BF16)
                lanes = slice(pair * 128, pair * 128 + 128)
                for q in range(16):
                    for which in range(2):
                        moved[which, q, pl.ds(cell, 16), lanes] = turned[
                            q * 16 : (q + 1) * 16, which * 128 : which * 128 + 128
                        ]
        for copy in departures(piece):
            copy.start()
        return carry

    lax.fori_loop(0, parts, turn, 0)
    for copy in small:
        copy.wait()
    values[...] = z[...].astype(BF16)
    lane = lax.broadcasted_iota(jnp.int32, (8, 128), 1)
    low_lane = lane < 64
    for which, out_ref in ((1 - core, send_ref), (core, keep_ref)):
        level = lane % 64 + 64 * which

        def factor(q):
            return jnp.dot(values[...], moved[which, q], preferred_element_type=F32)

        def live(pair, q):
            one = q + 32 * pair
            top = jnp.where(low_lane, ranks[one, tile], ranks[one + 16, tile])
            return (level < top).astype(F32)[:1]

        project(factor, quads, live, out_ref)

    def finish(piece, carry):
        for copy in departures(piece):
            copy.wait()
        return carry

    lax.fori_loop(0, parts, finish, 0)


def col_setup(factors, place, tile_ranks, z, coefficients):
    cells, tiles, ranked = factors.shape
    shape = (tiles // 4, cells, 2 * ranked)
    parts = 8
    return pl.pallas_call(
        col_setup_kernel,
        in_specs=[SMEM, ANY, ANY, ANY],
        out_specs=[ANY] * 2 + [VMEM] * 2,
        out_shape=[pltpu.HBM(shape, BF16)] * 2 + [jax.ShapeDtypeStruct(*coefficients)] * 2,
        scratch_shapes=[
            pltpu.VMEM((cells * tiles, ranked), BF16),
            pltpu.VMEM((2, *shape), BF16),
            pltpu.SMEM(tile_ranks.shape, jnp.int32),
            pltpu.VMEM(z.shape, F32),
            pltpu.VMEM(z.shape, BF16),
            pltpu.SemaphoreType.DMA((parts,)),
            pltpu.SemaphoreType.DMA((2, parts)),
            pltpu.SemaphoreType.DMA((2,)),
        ],
        compiler_params=pltpu.CompilerParams(vmem_limit_bytes=24 << 20),
        cost_estimate=pl.CostEstimate(
            flops=8_000_000_000, bytes_accessed=1 << 24, transcendentals=0
        ),
    )(place, in_hbm(factors.reshape(cells * tiles, ranked)), in_hbm(tile_ranks), in_hbm(z))


def row_setup_kernel(place_ref, own_raw_ref, other_raw_ref, out_ref, raw, moved, in_sems, out_sems):
    _, quads, cells, _ = moved.shape
    tiles = 4 * quads
    parts = in_sems.shape[1]
    step = cells // parts
    order = one_hot(tile_major)

    def arrival(side, piece):
        rows = pl.ds(pl.multiple_of(piece * step * tiles, 16), step * tiles)
        source = (own_raw_ref, other_raw_ref)[side]
        return pltpu.make_async_copy(
            source.at[rows], raw.at[side, rows], in_sems.at[side, piece]
        )

    def departure(side, piece):
        at = pl.ds(pl.multiple_of(piece * step, 16), step)
        return pltpu.make_async_copy(
            moved.at[side, :, at, :], out_ref.at[side, :, at, :], out_sems.at[side, piece]
        )

    for side in range(2):
        def launch(piece, carry):
            arrival(side, piece).start()
            return carry

        lax.fori_loop(0, parts, launch, 0)
    for which in range(2):
        @pl.when(place_ref[0] == which)
        def _():
            for side in range(2):
                def turn(piece, carry):
                    arrival(side, piece).wait()
                    for group in range(step // 16):
                        cell = pl.multiple_of(piece * step + group * 16, 16)
                        blocks = read_blocks(raw.at[side], cell, tiles)
                        both = jnp.concatenate(
                            [
                                half_lanes(*blocks[2 * pair : 2 * pair + 2], which)
                                for pair in range(2)
                            ],
                            axis=1,
                        )
                        turned = jnp.dot(
                            order, both, preferred_element_type=F32
                        ).astype(BF16)
                        for q in range(16):
                            moved[side, q, pl.ds(cell, 16), :] = turned[
                                q * 16 : (q + 1) * 16
                            ]
                    departure(side, piece).start()
                    return carry

                lax.fori_loop(0, parts, turn, 0)

    for side in range(2):
        def finish(piece, carry):
            departure(side, piece).wait()
            return carry

        lax.fori_loop(0, parts, finish, 0)


def row_setup(own, other, place):
    cells, tiles, ranked = own.shape
    shape = (2, tiles // 4, cells, 2 * ranked)
    parts = 8
    rows = (cells * tiles, ranked)
    return pl.pallas_call(
        row_setup_kernel,
        in_specs=[SMEM, ANY, ANY],
        out_specs=ANY,
        out_shape=pltpu.HBM(shape, BF16),
        scratch_shapes=[
            pltpu.VMEM((2, *rows), BF16),
            pltpu.VMEM(shape, BF16),
            pltpu.SemaphoreType.DMA((2, parts)),
            pltpu.SemaphoreType.DMA((2, parts)),
        ],
        compiler_params=pltpu.CompilerParams(vmem_limit_bytes=32 << 20),
        cost_estimate=pl.CostEstimate(
            flops=8_000_000_000, bytes_accessed=1 << 24, transcendentals=0
        ),
    )(place, in_hbm(own.reshape(rows)), in_hbm(other.reshape(rows)))


def merge_kernel(after_ref, *refs):
    sources, (out_ref, turned_ref, sems) = refs[:-3], refs[-3:]
    if len(sources) == 1:
        sources = sources[0].at[0], sources[0].at[1]
    quads, cells = out_ref.shape[1], out_ref.shape[2]
    size = quads // sems.shape[1]

    def copies(group):
        quad = pl.ds(group * size, size)
        return [
            pltpu.make_async_copy(
                source.at[quad], out_ref.at[side, quad], sems.at[side, group]
            )
            for side, source in enumerate(sources)
        ]

    def launch(group, carry):
        for copy in copies(group):
            copy.start()
        return carry

    lax.fori_loop(0, sems.shape[1], launch, 0)

    def turn(group, carry):
        for copy in copies(group):
            copy.wait()
        for q in range(size):
            quad = group * size + q
            for side in range(2):
                for block in range(cells // 256):
                    at_cell = slice(256 * block, 256 * block + 256)
                    turned_ref[side, quad, :, at_cell] = jnp.transpose(
                        out_ref[side, quad, at_cell, :]
                    )
        return carry

    lax.fori_loop(0, sems.shape[1], turn, 0)


def merge(after, *parts):
    quads, cells, lanes = parts[0].shape[-3:]
    return pl.pallas_call(
        merge_kernel,
        in_specs=[ANY] * (1 + len(parts)),
        out_specs=[VMEM] * 2,
        out_shape=[
            jax.ShapeDtypeStruct((2, quads, cells, lanes), BF16),
            jax.ShapeDtypeStruct((2, quads, lanes, cells), BF16),
        ],
        scratch_shapes=[pltpu.SemaphoreType.DMA((2, 8))],
        compiler_params=pltpu.CompilerParams(vmem_limit_bytes=4 << 20),
        cost_estimate=pl.CostEstimate(
            flops=4_000_000_000, bytes_accessed=1 << 24, transcendentals=0
        ),
    )(after, *[in_hbm(part) for part in parts])


def add_kernel(keep_ref, arrived_ref, out_ref):
    out_ref[...] = (keep_ref[...].astype(F32) + arrived_ref[...].astype(F32)).astype(BF16)


def expand_side(side, left_ref, turned_ref, total_ref):
    quads, cells = turned_ref.shape[1], turned_ref.shape[3]
    for block in range(cells // 256):
        at_cell = slice(256 * block, 256 * block + 256)
        total_ref[:, at_cell] = sum(
            jnp.dot(
                left_ref[q], turned_ref[side, q, :, at_cell], preferred_element_type=F32
            )
            for q in range(quads)
        )


def expand_first_kernel(side, coefficient_ref, turned_ref, total_ref, left_ref):
    quads, cells = turned_ref.shape[1], turned_ref.shape[3]
    blocks = [slice(256 * b, 256 * b + 256) for b in range(cells // 256)]
    totals = [0.0] * len(blocks)
    for q in range(quads):
        pairs = []
        for pair in range(2):
            one = coefficient_ref[q + 32 * pair]
            two = coefficient_ref[q + 32 * pair + 16]
            low = low_lanes(one)
            pairs.append(
                jnp.concatenate(
                    [
                        jnp.where(low, one, other_half(two)),
                        jnp.where(low, other_half(one), two),
                    ],
                    axis=0,
                )
            )
        left = jnp.concatenate(pairs, axis=1)
        left_ref[q] = left
        for b, at_cell in enumerate(blocks):
            totals[b] += jnp.dot(
                left, turned_ref[side, q, :, at_cell], preferred_element_type=F32
            )
    for b, at_cell in enumerate(blocks):
        total_ref[:, at_cell] = totals[b]


def project(factor, quads, live, out_ref):
    half = out_ref.shape[1]
    low = lax.broadcasted_iota(jnp.int32, (half, 128), 1) < 64

    def quad(q, carry):
        moved = factor(q)
        for pair in range(2):
            one, two = q + 32 * pair, q + 32 * pair + 16
            part = moved[:, pair * 128 : pair * 128 + 128] * live(pair, q)
            part = part.astype(BF16)
            turned = other_half(part)
            out_ref[one] = jnp.where(low, part[:half], turned[half:])
            out_ref[two] = jnp.where(low, turned[:half], part[half:])
        return carry

    lax.fori_loop(0, quads, quad, 0, unroll=UNROLL)


def row_values(total_ref, arrived_ref, base_ref, rate_ref, values):
    rate = rate_ref[...]
    exponent = base_ref[...] + (total_ref[...] + arrived_ref[...])
    intensity = jnp.exp(exponent)
    values[...] = (rate - intensity).astype(BF16)
    return intensity - rate * exponent


def col_values(
    weight, total_ref, arrived_ref, step_ref, z_ref, m_ref, state_refs, values
):
    step = step_ref[:, :1]
    z = z_ref[...]
    moment = m_ref[...] - weight * step * (z - (total_ref[...] + arrived_ref[...]))
    z = z + step * moment
    for ref, new in zip(state_refs, (z, moment)):
        ref[...] = new
    values[...] = z.astype(BF16)


def project_first(values, f_ref, part_ref):
    def quad(q, carry):
        part_ref[q] = jnp.dot(values[...], f_ref[1, q], preferred_element_type=F32)
        return carry

    lax.fori_loop(0, part_ref.shape[0], quad, 0, unroll=UNROLL)


def project_second(values, f_ref, part_ref, live_ref, out_ref):
    def factor(q):
        return part_ref[q] + jnp.dot(
            values[...], f_ref[0, q], preferred_element_type=F32
        )

    def live(pair, q):
        return live_ref[pair * 16 + q, :1]

    project(factor, part_ref.shape[0], live, out_ref)


def row_first_kernel(total_ref, arrived_ref, base_ref, rate_ref, f_ref, part_ref, values):
    row_values(total_ref, arrived_ref, base_ref, rate_ref, values)
    project_first(values, f_ref, part_ref)


def row_second_kernel(
    live_ref, total_ref, arrived_ref, base_ref, rate_ref, f_ref, part_ref, out_ref, *refs
):
    *energy_ref, values = refs
    energy = row_values(total_ref, arrived_ref, base_ref, rate_ref, values)
    if energy_ref:
        energy_ref[0][...] = jnp.sum(energy, axis=1, keepdims=True)
    project_second(values, f_ref, part_ref, live_ref, out_ref)


def col_first_kernel(
    weight, total_ref, arrived_ref, step_ref, z_ref, m_ref, f_ref, part_ref, *refs
):
    *state_refs, values = refs
    col_values(
        weight, total_ref, arrived_ref, step_ref, z_ref, m_ref, state_refs, values
    )
    project_first(values, f_ref, part_ref)


def col_second_kernel(
    weight, live_ref, total_ref, arrived_ref, step_ref, z_ref, m_ref, f_ref, part_ref,
    out_ref, new_z_ref, new_m_ref, values,
):
    col_values(
        weight, total_ref, arrived_ref, step_ref, z_ref, m_ref,
        (new_z_ref, new_m_ref), values,
    )
    project_second(values, f_ref, part_ref, live_ref, out_ref)


def last_kernel(
    total_ref, arrived_ref, step_ref, z_ref, m_ref, start_z_ref, start_m_ref,
    start_energy_ref, end_energy_ref, new_m_ref, change_ref,
):
    z = z_ref[...]
    moment = m_ref[...] - 0.5 * step_ref[:, :1] * (
        z - (total_ref[...] + arrived_ref[...])
    )
    new_m_ref[...] = moment
    start_z = start_z_ref[...]
    start_m = start_m_ref[...]
    pieces = 0.5 * (z * z - start_z * start_z + moment * moment - start_m * start_m)
    change = (
        jnp.sum(pieces, axis=1, keepdims=True) + end_energy_ref[...] - start_energy_ref[...]
    )
    row = jnp.transpose(jnp.broadcast_to(change, (change.shape[0], change.shape[0])))[:1]
    change_ref[...] = jnp.broadcast_to(row[None], change_ref.shape)


def call(kernel, specs, outs, scratch, flops, *args):
    return pl.pallas_call(
        kernel,
        in_specs=specs,
        out_specs=[VMEM] * len(outs),
        out_shape=[jax.ShapeDtypeStruct(*o) for o in outs],
        scratch_shapes=scratch,
        compiler_params=pltpu.CompilerParams(vmem_limit_bytes=LIMIT),
        cost_estimate=pl.CostEstimate(
            flops=flops, bytes_accessed=1 << 24, transcendentals=0
        ),
    )(*args)


def on_device(
    position, momentum, row_factors, col_factors, tile_ranks, log_mean, counts, step_size
):
    chains, cells = position.shape
    half = chains // 2
    tiles, ranked = tile_ranks.shape[0], row_factors.shape[2]
    tile = lax.axis_index(CHIPS)
    core = lax.axis_index(CORE).astype(jnp.int32)
    place = jnp.stack([core, tile.astype(jnp.int32)])
    lane = jnp.arange(ranked, dtype=jnp.int32)

    def live(ranks):
        tops = ranks.reshape(2, 2, tiles // 4)
        top = jnp.where(lane < ranked // 2, tops[:, 0, :, None], tops[:, 1, :, None])
        level = lane % (ranked // 2) + ranked // 2 * core
        alive = (level < top).astype(F32).reshape(tiles // 2, 1, ranked)
        return jnp.broadcast_to(alive, (tiles // 2, 8, ranked))

    coefficients = ((tiles, half, ranked), BF16)
    state = ((chains, cells), F32)
    part = ((tiles // 4, chains, 2 * ranked), F32)
    left = ((tiles // 4, chains, 2 * ranked), BF16)
    column = ((chains, 1), F32)
    values = [pltpu.VMEM((chains, cells), BF16)]
    work = 2 * chains * cells * tiles * ranked // 2

    row_arrived = swap(row_factors)
    col_own, col_sent, keep, send = col_setup(
        col_factors, place, tile_ranks, position, coefficients
    )
    sent = swap(send)
    (out,) = call(add_kernel, [VMEM] * 2, [coefficients], [], 1 << 24, keep, sent)
    out, col_sent, row_factors, tile_ranks, step_size = lax.optimization_barrier(
        (out, col_sent, row_factors, tile_ranks, step_size)
    )
    arrived = spread(out)
    row_whole = row_setup(row_factors, row_arrived, place)
    rate = counts.astype(F32)
    z_other, m_other = swap(position), swap(momentum)
    base_other, rate_other = swap(log_mean), swap(rate)
    col_other = swap(col_sent)
    col_live = live(lax.dynamic_slice_in_dim(tile_ranks, tile, 1, 1)[:, 0])
    row_live = live(lax.dynamic_slice_in_dim(tile_ranks, tile, 1, 0)[0])
    base = log_mean[None, :], base_other[None, :]
    rate = rate[None, :], rate_other[None, :]
    step = jnp.broadcast_to(step_size[:, None], (chains, ranked))

    def expand(coefficient, factors, first):
        one, rows = call(
            functools.partial(expand_first_kernel, first), [VMEM] * 2, [state, left], [],
            2 * work, coefficient, factors[1],
        )
        one_arrived = swap(one)
        (two,) = call(
            functools.partial(expand_side, 1 - first), [VMEM] * 2, [state], [],
            2 * work, rows, factors[1],
        )
        return one, two, one_arrived

    def row_pass(arrived, energy=True):
        own, other, for_other = expand(arrived, row, 0)
        for_own = swap(other)
        (share,) = call(
            row_first_kernel, [VMEM] * 5, [part], values, work,
            other, for_other, base[1], rate[1], row[0],
        )
        return call(
            row_second_kernel, [VMEM] * 7, [coefficients] + [column] * energy, values, work,
            row_live, own, for_own, base[0], rate[0], row[0], share,
        )

    def col_pass(weight, arrived, z, m, final=False):
        own, other, for_other = expand(arrived, col, 0)
        for_own = swap(other)
        share, *partner = call(
            functools.partial(col_first_kernel, weight), [VMEM] * 6,
            [part] + [state] * (0 if final else 2), values, work, other, for_other, step, z[1], m[1], col[0],
        )
        out, z_here, m_here = call(
            functools.partial(col_second_kernel, weight), [VMEM] * 8,
            [coefficients, state, state], values, work,
            col_live, own, for_own, step, z[0], m[0], col[0], share,
        )
        return out, (z_here, *partner[:1]), (m_here, *partner[1:])

    arrived, position, momentum, z_other, m_other, base, rate, step, row_live, col_live = (
        lax.optimization_barrier(
            (
                arrived, position, momentum, z_other, m_other,
                base, rate, step, row_live, col_live,
            )
        )
    )
    z, m = (position, z_other), (momentum, m_other)
    row = merge(arrived, row_whole)
    out, start_energy = row_pass(arrived)
    out, col_other = lax.optimization_barrier((out, col_other))
    arrived = spread(out)
    col = merge(arrived, col_own, col_other)
    out, z, m = col_pass(0.5, arrived, z, m)
    (out,) = row_pass(spread(out), False)
    out, z, m = col_pass(1.0, spread(out), z, m, final=True)
    out, end_energy = row_pass(spread(out))
    _, own, for_own = expand(spread(out), col, 1)
    m, change = call(
        last_kernel, [VMEM] * 9, [state, ((tiles, 1, chains), F32)], [], 1 << 24,
        own, for_own, step, z[0], m[0], position, momentum, start_energy, end_energy,
    )
    change = spread(change)
    change = change.sum(axis=(0, 1))
    change = change + swap(change)
    return z[0], m, change


def solution(mesh):
    split = Mesh(
        mesh.devices.reshape(4, 4, 4, 2), ("col_0", "col_1", "row_0", "row_1")
    )
    return jax.shard_map(
        on_device,
        mesh=split,
        in_specs=(
            P(None, COL_ROW),
            P(None, COL_ROW),
            P(COL_ROW, None, None),
            P(COL_ROW, None, None),
            P(),
            P(COL_ROW),
            P(COL_ROW),
            P(),
        ),
        out_specs=(P(None, COL_ROW), P(None, COL_ROW), P()),
        check_vma=False,
    )
```

```python
import functools

import jax
import jax.numpy as jnp
from jax import lax
from jax.experimental import pallas as pl
from jax.experimental.pallas import tpu as pltpu
from jax.sharding import Mesh
from jax.sharding import PartitionSpec as P

COL_ROW = ("col_0", "col_1", "row_0", "row_1")
CHIPS = ("col_0", "col_1", "row_0")
CORE = "row_1"
BF16 = jnp.bfloat16
F32 = jnp.float32
LIMIT = 8 << 20
UNROLL = 8
VMEM = pl.BlockSpec(memory_space=pltpu.VMEM)
SMEM = pl.BlockSpec(memory_space=pltpu.SMEM)
ANY = pl.BlockSpec(memory_space=pl.ANY)


def swap(value):
    return lax.ppermute(value, CORE, [(0, 1), (1, 0)])


def spread(value):
    return lax.all_to_all(value, CHIPS, split_axis=0, concat_axis=0, tiled=True)


def in_hbm(value):
    return pltpu.with_memory_space_constraint(value, pltpu.HBM)


def other_half(value):
    lanes = value.shape[1] // 2
    return jnp.concatenate([value[:, lanes:], value[:, :lanes]], axis=1)


def low_lanes(value):
    return lax.broadcasted_iota(jnp.int32, value.shape, 1) < value.shape[1] // 2


def one_hot(index):
    to = lax.broadcasted_iota(jnp.int32, (256, 256), 0)
    at = lax.broadcasted_iota(jnp.int32, (256, 256), 1)
    return (at == index(to)).astype(F32).astype(BF16)


def tile_major(to):
    return (to % 16) * 16 + to // 16


def read_blocks(raw, cell, tiles):
    return [
        jnp.concatenate(
            [
                raw[pl.ds(pl.multiple_of((cell + y) * tiles + block * 16, 16), 16), :]
                for y in range(16)
            ],
            axis=0,
        )
        for block in range(tiles // 16)
    ]


def half_lanes(one, two, which):
    low = low_lanes(one)
    if which == 0:
        return jnp.where(low, one, other_half(two))
    return jnp.where(low, other_half(one), two)


def col_setup_kernel(
    place_ref, raw_ref, ranks_ref, z_ref, own_ref, sent_ref, keep_ref, send_ref,
    raw, moved, ranks, z, values, in_sems, out_sems, small_sems,
):
    _, quads, cells, _ = moved.shape
    tiles = 4 * quads
    parts = in_sems.shape[0]
    step = cells // parts
    core, tile = place_ref[0], place_ref[1]

    def arrival(piece):
        rows = pl.ds(pl.multiple_of(piece * step * tiles, 16), step * tiles)
        return pltpu.make_async_copy(raw_ref.at[rows], raw.at[rows], in_sems.at[piece])

    def departures(piece):
        at = pl.ds(pl.multiple_of(piece * step, 16), step)
        return [
            pltpu.make_async_copy(
                moved.at[which, :, at, :], ref.at[:, at, :], out_sems.at[side, piece]
            )
            for side, (which, ref) in enumerate(((core, own_ref), (1 - core, sent_ref)))
        ]

    def launch(piece, carry):
        arrival(piece).start()
        return carry

    lax.fori_loop(0, parts, launch, 0)
    small = [
        pltpu.make_async_copy(z_ref, z, small_sems.at[0]),
        pltpu.make_async_copy(ranks_ref, ranks, small_sems.at[1]),
    ]
    for copy in small:
        copy.start()
    order = one_hot(tile_major)

    def turn(piece, carry):
        arrival(piece).wait()
        for group in range(step // 16):
            cell = pl.multiple_of(piece * step + group * 16, 16)
            blocks = read_blocks(raw, cell, tiles)
            for pair in range(2):
                one, two = blocks[2 * pair : 2 * pair + 2]
                both = jnp.concatenate(
                    [half_lanes(one, two, 0), half_lanes(one, two, 1)], axis=1
                )
                turned = jnp.dot(order, both, preferred_element_type=F32).astype(BF16)
                lanes = slice(pair * 128, pair * 128 + 128)
                for q in range(16):
                    for which in range(2):
                        moved[which, q, pl.ds(cell, 16), lanes] = turned[
                            q * 16 : (q + 1) * 16, which * 128 : which * 128 + 128
                        ]
        for copy in departures(piece):
            copy.start()
        return carry

    lax.fori_loop(0, parts, turn, 0)
    for copy in small:
        copy.wait()
    values[...] = z[...].astype(BF16)
    lane = lax.broadcasted_iota(jnp.int32, (8, 128), 1)
    low_lane = lane < 64
    for which, out_ref in ((1 - core, send_ref), (core, keep_ref)):
        level = lane % 64 + 64 * which

        def factor(q):
            return jnp.dot(values[...], moved[which, q], preferred_element_type=F32)

        def live(pair, q):
            one = q + 32 * pair
            top = jnp.where(low_lane, ranks[one, tile], ranks[one + 16, tile])
            return (level < top).astype(F32)[:1]

        project(factor, quads, live, out_ref)

    def finish(piece, carry):
        for copy in departures(piece):
            copy.wait()
        return carry

    lax.fori_loop(0, parts, finish, 0)


def col_setup(factors, place, tile_ranks, z, coefficients):
    cells, tiles, ranked = factors.shape
    shape = (tiles // 4, cells, 2 * ranked)
    parts = 16
    return pl.pallas_call(
        col_setup_kernel,
        in_specs=[SMEM, ANY, ANY, ANY],
        out_specs=[ANY] * 2 + [VMEM] * 2,
        out_shape=[pltpu.HBM(shape, BF16)] * 2 + [jax.ShapeDtypeStruct(*coefficients)] * 2,
        scratch_shapes=[
            pltpu.VMEM((cells * tiles, ranked), BF16),
            pltpu.VMEM((2, *shape), BF16),
            pltpu.SMEM(tile_ranks.shape, jnp.int32),
            pltpu.VMEM(z.shape, F32),
            pltpu.VMEM(z.shape, BF16),
            pltpu.SemaphoreType.DMA((parts,)),
            pltpu.SemaphoreType.DMA((2, parts)),
            pltpu.SemaphoreType.DMA((2,)),
        ],
        compiler_params=pltpu.CompilerParams(vmem_limit_bytes=24 << 20),
        cost_estimate=pl.CostEstimate(
            flops=8_000_000_000, bytes_accessed=1 << 24, transcendentals=0
        ),
    )(place, in_hbm(factors.reshape(cells * tiles, ranked)), in_hbm(tile_ranks), in_hbm(z))


def row_setup_kernel(place_ref, own_raw_ref, other_raw_ref, out_ref, raw, moved, in_sems, out_sems):
    _, quads, cells, _ = moved.shape
    tiles = 4 * quads
    parts = in_sems.shape[1]
    step = cells // parts
    order = one_hot(tile_major)

    def arrival(side, piece):
        rows = pl.ds(pl.multiple_of(piece * step * tiles, 16), step * tiles)
        source = (own_raw_ref, other_raw_ref)[side]
        return pltpu.make_async_copy(
            source.at[rows], raw.at[side, rows], in_sems.at[side, piece]
        )

    def departure(side, piece):
        at = pl.ds(pl.multiple_of(piece * step, 16), step)
        return pltpu.make_async_copy(
            moved.at[side, :, at, :], out_ref.at[side, :, at, :], out_sems.at[side, piece]
        )

    for side in range(2):
        def launch(piece, carry):
            arrival(side, piece).start()
            return carry

        lax.fori_loop(0, parts, launch, 0)
    for which in range(2):
        @pl.when(place_ref[0] == which)
        def _():
            for side in range(2):
                def turn(piece, carry):
                    arrival(side, piece).wait()
                    for group in range(step // 16):
                        cell = pl.multiple_of(piece * step + group * 16, 16)
                        blocks = read_blocks(raw.at[side], cell, tiles)
                        both = jnp.concatenate(
                            [
                                half_lanes(*blocks[2 * pair : 2 * pair + 2], which)
                                for pair in range(2)
                            ],
                            axis=1,
                        )
                        turned = jnp.dot(
                            order, both, preferred_element_type=F32
                        ).astype(BF16)
                        for q in range(16):
                            moved[side, q, pl.ds(cell, 16), :] = turned[
                                q * 16 : (q + 1) * 16
                            ]
                    departure(side, piece).start()
                    return carry

                lax.fori_loop(0, parts, turn, 0)

    for side in range(2):
        def finish(piece, carry):
            departure(side, piece).wait()
            return carry

        lax.fori_loop(0, parts, finish, 0)


def row_setup(own, other, place):
    cells, tiles, ranked = own.shape
    shape = (2, tiles // 4, cells, 2 * ranked)
    parts = 16
    rows = (cells * tiles, ranked)
    return pl.pallas_call(
        row_setup_kernel,
        in_specs=[SMEM, ANY, ANY],
        out_specs=ANY,
        out_shape=pltpu.HBM(shape, BF16),
        scratch_shapes=[
            pltpu.VMEM((2, *rows), BF16),
            pltpu.VMEM(shape, BF16),
            pltpu.SemaphoreType.DMA((2, parts)),
            pltpu.SemaphoreType.DMA((2, parts)),
        ],
        compiler_params=pltpu.CompilerParams(vmem_limit_bytes=32 << 20),
        cost_estimate=pl.CostEstimate(
            flops=8_000_000_000, bytes_accessed=1 << 24, transcendentals=0
        ),
    )(place, in_hbm(own.reshape(rows)), in_hbm(other.reshape(rows)))


def merge_kernel(after_ref, *refs):
    sources, (out_ref, turned_ref, sems) = refs[:-3], refs[-3:]
    if len(sources) == 1:
        sources = sources[0].at[0], sources[0].at[1]
    quads, cells = out_ref.shape[1], out_ref.shape[2]
    size = quads // sems.shape[1]

    def copies(group):
        quad = pl.ds(group * size, size)
        return [
            pltpu.make_async_copy(
                source.at[quad], out_ref.at[side, quad], sems.at[side, group]
            )
            for side, source in enumerate(sources)
        ]

    def launch(group, carry):
        for copy in copies(group):
            copy.start()
        return carry

    lax.fori_loop(0, sems.shape[1], launch, 0)

    def turn(group, carry):
        for copy in copies(group):
            copy.wait()
        for q in range(size):
            quad = group * size + q
            for side in range(2):
                for block in range(cells // 256):
                    at_cell = slice(256 * block, 256 * block + 256)
                    turned_ref[side, quad, :, at_cell] = jnp.transpose(
                        out_ref[side, quad, at_cell, :]
                    )
        return carry

    lax.fori_loop(0, sems.shape[1], turn, 0)


def merge(after, *parts):
    quads, cells, lanes = parts[0].shape[-3:]
    return pl.pallas_call(
        merge_kernel,
        in_specs=[ANY] * (1 + len(parts)),
        out_specs=[VMEM] * 2,
        out_shape=[
            jax.ShapeDtypeStruct((2, quads, cells, lanes), BF16),
            jax.ShapeDtypeStruct((2, quads, lanes, cells), BF16),
        ],
        scratch_shapes=[pltpu.SemaphoreType.DMA((2, 16))],
        compiler_params=pltpu.CompilerParams(vmem_limit_bytes=4 << 20),
        cost_estimate=pl.CostEstimate(
            flops=4_000_000_000, bytes_accessed=1 << 24, transcendentals=0
        ),
    )(after, *[in_hbm(part) for part in parts])


def add_kernel(keep_ref, arrived_ref, out_ref):
    out_ref[...] = (keep_ref[...].astype(F32) + arrived_ref[...].astype(F32)).astype(BF16)


def expand_side(side, left_ref, turned_ref, total_ref):
    quads, cells = turned_ref.shape[1], turned_ref.shape[3]
    for block in range(cells // 256):
        at_cell = slice(256 * block, 256 * block + 256)
        total_ref[:, at_cell] = sum(
            jnp.dot(
                left_ref[q], turned_ref[side, q, :, at_cell], preferred_element_type=F32
            )
            for q in range(quads)
        )


def expand_first_kernel(side, coefficient_ref, turned_ref, total_ref, left_ref):
    quads, cells = turned_ref.shape[1], turned_ref.shape[3]
    blocks = [slice(256 * b, 256 * b + 256) for b in range(cells // 256)]
    totals = [0.0] * len(blocks)
    for q in range(quads):
        pairs = []
        for pair in range(2):
            one = coefficient_ref[q + 32 * pair]
            two = coefficient_ref[q + 32 * pair + 16]
            low = low_lanes(one)
            pairs.append(
                jnp.concatenate(
                    [
                        jnp.where(low, one, other_half(two)),
                        jnp.where(low, other_half(one), two),
                    ],
                    axis=0,
                )
            )
        left = jnp.concatenate(pairs, axis=1)
        left_ref[q] = left
        for b, at_cell in enumerate(blocks):
            totals[b] += jnp.dot(
                left, turned_ref[side, q, :, at_cell], preferred_element_type=F32
            )
    for b, at_cell in enumerate(blocks):
        total_ref[:, at_cell] = totals[b]


def project(factor, quads, live, out_ref):
    half = out_ref.shape[1]
    low = lax.broadcasted_iota(jnp.int32, (half, 128), 1) < 64

    def quad(q, carry):
        moved = factor(q)
        for pair in range(2):
            one, two = q + 32 * pair, q + 32 * pair + 16
            part = moved[:, pair * 128 : pair * 128 + 128] * live(pair, q)
            part = part.astype(BF16)
            turned = other_half(part)
            out_ref[one] = jnp.where(low, part[:half], turned[half:])
            out_ref[two] = jnp.where(low, turned[:half], part[half:])
        return carry

    lax.fori_loop(0, quads, quad, 0, unroll=UNROLL)


def row_values(total_ref, arrived_ref, base_ref, rate_ref, values):
    rate = rate_ref[...]
    exponent = base_ref[...] + (total_ref[...] + arrived_ref[...])
    intensity = jnp.exp(exponent)
    values[...] = (rate - intensity).astype(BF16)
    return intensity - rate * exponent


def col_values(
    weight, total_ref, arrived_ref, step_ref, z_ref, m_ref, state_refs, values
):
    step = step_ref[:, :1]
    z = z_ref[...]
    moment = m_ref[...] - weight * step * (z - (total_ref[...] + arrived_ref[...]))
    z = z + step * moment
    for ref, new in zip(state_refs, (z, moment)):
        ref[...] = new
    values[...] = z.astype(BF16)


def project_first(values, f_ref, part_ref):
    def quad(q, carry):
        part_ref[q] = jnp.dot(values[...], f_ref[1, q], preferred_element_type=F32)
        return carry

    lax.fori_loop(0, part_ref.shape[0], quad, 0, unroll=UNROLL)


def project_second(values, f_ref, part_ref, live_ref, out_ref):
    def factor(q):
        return part_ref[q] + jnp.dot(
            values[...], f_ref[0, q], preferred_element_type=F32
        )

    def live(pair, q):
        return live_ref[pair * 16 + q, :1]

    project(factor, part_ref.shape[0], live, out_ref)


def row_first_kernel(total_ref, arrived_ref, base_ref, rate_ref, f_ref, part_ref, values):
    row_values(total_ref, arrived_ref, base_ref, rate_ref, values)
    project_first(values, f_ref, part_ref)


def row_second_kernel(
    live_ref, total_ref, arrived_ref, base_ref, rate_ref, f_ref, part_ref, out_ref, *refs
):
    *energy_ref, values = refs
    energy = row_values(total_ref, arrived_ref, base_ref, rate_ref, values)
    if energy_ref:
        energy_ref[0][...] = jnp.sum(energy, axis=1, keepdims=True)
    project_second(values, f_ref, part_ref, live_ref, out_ref)


def col_first_kernel(
    weight, total_ref, arrived_ref, step_ref, z_ref, m_ref, f_ref, part_ref, *refs
):
    *state_refs, values = refs
    col_values(
        weight, total_ref, arrived_ref, step_ref, z_ref, m_ref, state_refs, values
    )
    project_first(values, f_ref, part_ref)


def col_second_kernel(
    weight, live_ref, total_ref, arrived_ref, step_ref, z_ref, m_ref, f_ref, part_ref,
    out_ref, new_z_ref, new_m_ref, values,
):
    col_values(
        weight, total_ref, arrived_ref, step_ref, z_ref, m_ref,
        (new_z_ref, new_m_ref), values,
    )
    project_second(values, f_ref, part_ref, live_ref, out_ref)


def last_kernel(
    total_ref, arrived_ref, step_ref, z_ref, m_ref, start_z_ref, start_m_ref,
    start_energy_ref, end_energy_ref, new_m_ref, change_ref,
):
    z = z_ref[...]
    moment = m_ref[...] - 0.5 * step_ref[:, :1] * (
        z - (total_ref[...] + arrived_ref[...])
    )
    new_m_ref[...] = moment
    start_z = start_z_ref[...]
    start_m = start_m_ref[...]
    pieces = 0.5 * (z * z - start_z * start_z + moment * moment - start_m * start_m)
    change = (
        jnp.sum(pieces, axis=1, keepdims=True) + end_energy_ref[...] - start_energy_ref[...]
    )
    row = jnp.transpose(jnp.broadcast_to(change, (change.shape[0], change.shape[0])))[:1]
    change_ref[...] = jnp.broadcast_to(row[None], change_ref.shape)


def call(kernel, specs, outs, scratch, flops, *args):
    return pl.pallas_call(
        kernel,
        in_specs=specs,
        out_specs=[VMEM] * len(outs),
        out_shape=[jax.ShapeDtypeStruct(*o) for o in outs],
        scratch_shapes=scratch,
        compiler_params=pltpu.CompilerParams(vmem_limit_bytes=LIMIT),
        cost_estimate=pl.CostEstimate(
            flops=flops, bytes_accessed=1 << 24, transcendentals=0
        ),
    )(*args)


def on_device(
    position, momentum, row_factors, col_factors, tile_ranks, log_mean, counts, step_size
):
    chains, cells = position.shape
    half = chains // 2
    tiles, ranked = tile_ranks.shape[0], row_factors.shape[2]
    tile = lax.axis_index(CHIPS)
    core = lax.axis_index(CORE).astype(jnp.int32)
    place = jnp.stack([core, tile.astype(jnp.int32)])
    lane = jnp.arange(ranked, dtype=jnp.int32)

    def live(ranks):
        tops = ranks.reshape(2, 2, tiles // 4)
        top = jnp.where(lane < ranked // 2, tops[:, 0, :, None], tops[:, 1, :, None])
        level = lane % (ranked // 2) + ranked // 2 * core
        alive = (level < top).astype(F32).reshape(tiles // 2, 1, ranked)
        return jnp.broadcast_to(alive, (tiles // 2, 8, ranked))

    coefficients = ((tiles, half, ranked), BF16)
    state = ((chains, cells), F32)
    part = ((tiles // 4, chains, 2 * ranked), F32)
    left = ((tiles // 4, chains, 2 * ranked), BF16)
    column = ((chains, 1), F32)
    values = [pltpu.VMEM((chains, cells), BF16)]
    work = 2 * chains * cells * tiles * ranked // 2

    row_arrived = swap(row_factors)
    col_own, col_sent, keep, send = col_setup(
        col_factors, place, tile_ranks, position, coefficients
    )
    sent = swap(send)
    (out,) = call(add_kernel, [VMEM] * 2, [coefficients], [], 1 << 24, keep, sent)
    out, col_sent, row_factors, tile_ranks, step_size = lax.optimization_barrier(
        (out, col_sent, row_factors, tile_ranks, step_size)
    )
    arrived = spread(out)
    row_whole = row_setup(row_factors, row_arrived, place)
    rate = counts.astype(F32)
    z_other, m_other = swap(position), swap(momentum)
    base_other, rate_other = swap(log_mean), swap(rate)
    col_other = swap(col_sent)
    col_live = live(lax.dynamic_slice_in_dim(tile_ranks, tile, 1, 1)[:, 0])
    row_live = live(lax.dynamic_slice_in_dim(tile_ranks, tile, 1, 0)[0])
    base = log_mean[None, :], base_other[None, :]
    rate = rate[None, :], rate_other[None, :]
    step = jnp.broadcast_to(step_size[:, None], (chains, ranked))

    def expand(coefficient, factors, first):
        one, rows = call(
            functools.partial(expand_first_kernel, first), [VMEM] * 2, [state, left], [],
            2 * work, coefficient, factors[1],
        )
        one_arrived = swap(one)
        (two,) = call(
            functools.partial(expand_side, 1 - first), [VMEM] * 2, [state], [],
            2 * work, rows, factors[1],
        )
        return one, two, one_arrived

    def row_pass(arrived, energy=True):
        own, other, for_other = expand(arrived, row, 0)
        for_own = swap(other)
        (share,) = call(
            row_first_kernel, [VMEM] * 5, [part], values, work,
            other, for_other, base[1], rate[1], row[0],
        )
        return call(
            row_second_kernel, [VMEM] * 7, [coefficients] + [column] * energy, values, work,
            row_live, own, for_own, base[0], rate[0], row[0], share,
        )

    def col_pass(weight, arrived, z, m, final=False):
        own, other, for_other = expand(arrived, col, 0)
        for_own = swap(other)
        share, *partner = call(
            functools.partial(col_first_kernel, weight), [VMEM] * 6,
            [part] + [state] * (0 if final else 2), values, work, other, for_other, step, z[1], m[1], col[0],
        )
        out, z_here, m_here = call(
            functools.partial(col_second_kernel, weight), [VMEM] * 8,
            [coefficients, state, state], values, work,
            col_live, own, for_own, step, z[0], m[0], col[0], share,
        )
        return out, (z_here, *partner[:1]), (m_here, *partner[1:])

    arrived, position, momentum, z_other, m_other, base, rate, step, row_live, col_live = (
        lax.optimization_barrier(
            (
                arrived, position, momentum, z_other, m_other,
                base, rate, step, row_live, col_live,
            )
        )
    )
    z, m = (position, z_other), (momentum, m_other)
    row = merge(arrived, row_whole)
    out, start_energy = row_pass(arrived)
    out, col_other = lax.optimization_barrier((out, col_other))
    arrived = spread(out)
    col = merge(arrived, col_own, col_other)
    out, z, m = col_pass(0.5, arrived, z, m)
    (out,) = row_pass(spread(out), False)
    out, z, m = col_pass(1.0, spread(out), z, m, final=True)
    out, end_energy = row_pass(spread(out))
    _, own, for_own = expand(spread(out), col, 1)
    m, change = call(
        last_kernel, [VMEM] * 9, [state, ((tiles, 1, chains), F32)], [], 1 << 24,
        own, for_own, step, z[0], m[0], position, momentum, start_energy, end_energy,
    )
    change = spread(change)
    change = change.sum(axis=(0, 1))
    change = change + swap(change)
    return z[0], m, change


def solution(mesh):
    split = Mesh(
        mesh.devices.reshape(4, 4, 4, 2), ("col_0", "col_1", "row_0", "row_1")
    )
    return jax.shard_map(
        on_device,
        mesh=split,
        in_specs=(
            P(None, COL_ROW),
            P(None, COL_ROW),
            P(COL_ROW, None, None),
            P(COL_ROW, None, None),
            P(),
            P(COL_ROW),
            P(COL_ROW),
            P(),
        ),
        out_specs=(P(None, COL_ROW), P(None, COL_ROW), P()),
        check_vma=False,
    )
```
